256 devices in a mesh: batch: 4 (over x), proto: 64 (over y, z, core).
Axes of the slice: x: 4, y: 4, z: 8, core: 2. Of those that a mesh axis runs over, the one named last changes fastest.
Arguments:
- view_codes: bfloat16 [4096, 1024], P('batch', 'proto'), may hold values from -80 to 80
- predictor_view_embeddings: bfloat16 [4096, 1024], P('batch', 'proto'), may hold values from -80 to 80
- prototypes: bfloat16 [65536, 1024], P('proto'), may hold values from -64 to 64
Outputs:
- assignments: bfloat16 [4096, 65536], P('batch', 'proto')
- loss_rows: float32 [4096], P('batch')
The draws below stay inside these ranges and needn't reach their ends.
All inputs are finite; a program needn't handle non-finite values.
Results may differ from the reference program's by a relative error of at most 0.0034.
Values may be sent and summed in bfloat16 or wider, within the bound.
A program may use at most 64 MiB of HBM per device.

```python
import jax
import jax.numpy as jnp
from jax import lax

D = 1024
PROTOS = 65536
SINK_ITERS = 3
BATCH = 4096


def shared_centres(key):
    base_key = jax.random.fold_in(key, 17)
    keys = jax.random.split(base_key, 3)
    groups = PROTOS // 16
    centres = jax.random.truncated_normal(keys[0], -3.0, 3.0, (groups, D), jnp.float32)
    labels = jax.random.randint(keys[1], (BATCH,), 0, groups)
    owners = jax.random.randint(keys[2], (PROTOS,), 0, groups)
    return (centres, labels, owners)


def shared_views(key):
    centres, labels, owners = shared_centres(key)
    keys = jax.random.split(jax.random.fold_in(key, 29), 6)
    chosen = centres[labels]
    noise_first = jax.random.truncated_normal(keys[2], -4.0, 4.0, (BATCH, D), jnp.float32)
    noise_second = jax.random.truncated_normal(keys[3], -4.0, 4.0, (BATCH, D), jnp.float32)
    scale_first = jnp.exp(jax.random.uniform(keys[4], (BATCH, 1), jnp.float32, 0.0, 2.3))
    scale_second = jnp.exp(jax.random.uniform(keys[5], (BATCH, 1), jnp.float32, 0.0, 2.3))
    first = (chosen + 0.6 * noise_first) * scale_first
    second = (chosen + 0.6 * noise_second) * scale_second
    return (first, second)


def draw_view_codes(key, part):
    return shared_views(key)[0].astype(jnp.bfloat16)


def draw_predictor_view_embeddings(key, part):
    return shared_views(key)[1].astype(jnp.bfloat16)


def draw_prototypes(key, part):
    centres, labels, owners = shared_centres(key)
    keys = jax.random.split(jax.random.fold_in(key, 31), 2)
    chosen = centres[owners]
    noise = jax.random.truncated_normal(keys[0], -4.0, 4.0, (PROTOS, D), jnp.float32)
    scale = jnp.exp(jax.random.uniform(keys[1], (PROTOS, 1), jnp.float32, 0.0, 2.3))
    return ((chosen + 0.6 * noise) * scale).astype(jnp.bfloat16)


def setup_inputs(seed: int = 0) -> dict:
    streams_of = jax.random.split(jax.random.key(seed), 4)
    return {
        "view_codes": draw_view_codes(jax.random.fold_in(streams_of[3], 71), 0),
        "predictor_view_embeddings": draw_predictor_view_embeddings(jax.random.fold_in(streams_of[3], 71), 0),
        "prototypes": draw_prototypes(jax.random.fold_in(streams_of[3], 71), 0),
    }


EPSILON = 0.05
SOFTMAX_TEMP_VALUE = 0.1

def unit_protos(prototypes):
    weights = prototypes.astype(jnp.float32)
    return (weights * lax.rsqrt(lax.optimization_barrier(jnp.sum(weights * weights, axis=1, keepdims=True)) + 1e-06)).astype(jnp.bfloat16)

def tempered_scores(view, unit_prototype_rows):
    products = jnp.dot(view, unit_prototype_rows.T, preferred_element_type=jnp.float32)
    values = view.astype(jnp.float32)
    inverse_factor = lax.rsqrt(lax.optimization_barrier(jnp.sum(values * values, axis=1)) + 1e-06)
    return products * inverse_factor[:, None]

def reference(view_codes, predictor_view_embeddings, prototypes):
    unit_prototype_rows = unit_protos(prototypes)
    kernel = jnp.exp(tempered_scores(view_codes, unit_prototype_rows) / EPSILON)
    total_rows = kernel.shape[0]
    total_protos = kernel.shape[1]
    scale_rows = jnp.ones((total_rows,), jnp.float32)
    for iteration in range(SINK_ITERS):
        col_sums = jnp.dot(scale_rows, kernel, precision=lax.Precision.HIGHEST)
        scale_cols = 1.0 / (total_protos * col_sums)
        row_sums = jnp.dot(kernel, scale_cols, precision=lax.Precision.HIGHEST)
        scale_rows = 1.0 / (total_rows * row_sums)
    assign = kernel * scale_cols[None, :] * (total_rows * scale_rows)[:, None]
    assignments = (total_protos * assign).astype(jnp.bfloat16)
    logit_scores = tempered_scores(predictor_view_embeddings, unit_prototype_rows) / SOFTMAX_TEMP_VALUE
    totals = lax.optimization_barrier(jnp.sum(jnp.exp(logit_scores), axis=1))
    cross_term = lax.optimization_barrier(jnp.sum(assign * logit_scores, axis=1))
    loss_rows = jnp.log(totals) - cross_term
    return (assignments, loss_rows)
```

```python
import functools
import math

import jax
import jax.numpy as jnp
from jax import lax
from jax.experimental import pallas as pl
from jax.experimental.pallas import tpu as pltpu
from jax.sharding import PartitionSpec as P

SINK_ITERS = 3
EPSILON = 0.05
SOFTMAX_TEMP_VALUE = 0.1
LOG2E = math.log2(math.e)

MESH = pl.DeviceIdType.MESH
NX, NY, NZ = 4, 4, 8
NCHIP = NY * NZ
ROWS = 1024
COLS = 1024
DIM = 1024
SHARD = 16
LANES = 128
TOTAL_ROWS = 4096
TOTAL_PROTOS = 65536


def swap_kernel(
    v1_ref, v2_ref, p_ref, out_ref, loss_ref,
    xg, xp, praw, pu, kern, s2, xb, col_r, inv_col,
    colbuf, rowbuf, xbuf, cvec, svec, rvec, lvec, sstat, pstat, inv_row2,
    local_sem, stage_sem, gather_rs, send_sem, xp_rs, pu_rs, col_rs, row_rs, x_rs, vec_rs,
):
    b = lax.axis_index("batch")
    q = lax.axis_index("proto")
    c = q % 2
    z = (q // 2) % NZ
    y = q // (2 * NZ)
    chip = y * NZ + z

    def device(bb, yy, zz, cc):
        return (bb, yy * (2 * NZ) + zz * 2 + cc)

    def at_y(d):
        return device(b, (y + d) % NY, z, c)

    def at_z(d):
        return device(b, y, (z + d) % NZ, c)

    partner = device(b, y, z, 1 - c)
    sent = []

    def remote(src, dst, rsem, dev):
        return pltpu.make_async_remote_copy(
            src_ref=src, dst_ref=dst, send_sem=send_sem, recv_sem=rsem,
            device_id=dev, device_id_type=MESH)

    def start(src, dst, rsem, dev):
        copy = remote(src, dst, rsem, dev)
        copy.start()
        sent.append(copy)

    def drain():
        for copy in sent:
            copy.wait_send()
        sent.clear()

    own_p = pltpu.make_async_copy(p_ref, praw, local_sem.at[0])
    own_p.start()

    barrier = pltpu.get_barrier_semaphore()
    greet = [partner]
    greet += [device((b + d) % NX, y, z, c) for d in range(1, NX)]
    greet += [at_y(d) for d in range(1, NY)]
    greet += [at_z(d) for d in range(1, NZ)]
    for dev in greet:
        pl.semaphore_signal(barrier, 1, device_id=dev, device_id_type=MESH)
    pl.semaphore_wait(barrier, len(greet))

    def normalize(slot):
        own_p.wait()

        def body(i, _):
            rows = pl.ds(pl.multiple_of(i * 64, 64), 64)
            w = praw[rows, :].astype(jnp.float32)
            total = jnp.sum(w * w, axis=1, keepdims=True)
            pu[slot, rows, :] = (w * lax.rsqrt(total + 1e-06)).astype(jnp.bfloat16)
            return 0

        lax.fori_loop(0, ROWS // 64, body, 0)

    def put(yy, zz, h, dev):
        start(xg.at[yy, zz, h], xg.at[yy, zz, h], gather_rs.at[yy, zz, h], dev)

    def arrived(yy, zz, h):
        remote(xg.at[yy, zz, h], xg.at[yy, zz, h], gather_rs.at[yy, zz, h], partner).wait_recv()

    def hops(j, direction):
        far = NZ // 2
        if direction > 0:
            return far if j in (0, 1) else far - 1
        return far - 1 if j in (0, 1) else far

    def gather():
        def yj(j):
            return (y + j) % NY

        def zk(k):
            return (z + k) % NZ

        for d in (2, 1, 3):
            put(y, z, 0, at_y(d))
        for h in (0, 1):
            put(y, z, h, at_z(1))
            put(y, z, h, at_z(-1 + NZ))
        for d in (2, 1, 3):
            put(y, z, 1, at_y(d))

        def ring(k, js):
            for direction in (1, -1):
                zz = zk(NZ - k) if direction > 0 else zk(k)
                nxt = at_z(1) if direction > 0 else at_z(NZ - 1)
                for j in js:
                    if hops(j, direction) >= k:
                        arrived(yj(j), zz, 0)
                        if hops(j, direction) > k:
                            put(yj(j), zz, 0, nxt)
                    if j == 0 and hops(1, direction) >= k:
                        arrived(y, zz, 1)
                        if hops(1, direction) > k:
                            put(y, zz, 1, nxt)
                        for d in (2, 1, 3):
                            put(y, zz, 1, at_y(d))

        far = NZ // 2
        ring(1, (0,))
        for j in (1, 3, 2):
            arrived(yj(j), z, 0)
            put(yj(j), z, 0, at_z(1))
            put(yj(j), z, 0, at_z(NZ - 1))
        for k in range(1, far + 1):
            if k < far:
                ring(k + 1, (0,))
            ring(k, (1, 3, 2))
        for zz in range(NZ):
            for j in (1, 2, 3):
                arrived(yj(j), zk(zz), 1)

    def inverse_norms(xt):
        def body(s, acc):
            v = xt[s // NZ, s % NZ].reshape(2 * SHARD, ROWS).astype(jnp.float32)
            return acc + v * v

        acc = lax.fori_loop(0, NCHIP, body, jnp.zeros((2 * SHARD, ROWS), jnp.float32))
        return lax.rsqrt(jnp.sum(acc, axis=0, keepdims=True) + 1e-06)

    def spread(row, dst, g):
        dst[g * LANES:(g + 1) * LANES, :] = jnp.transpose(
            jnp.broadcast_to(row, (LANES, LANES)))

    def transpose_view(xt):
        for kb in range(DIM // LANES):
            yy, z0 = kb // 2, (kb % 2) * 4
            block = xt[yy, z0:z0 + 4].reshape(LANES, ROWS)
            xb[:, kb * LANES:(kb + 1) * LANES] = jnp.transpose(block)

    MB, NB = 512, 256

    def products(slot, n0, epilogue):
        def body(i, _):
            nrows = pl.ds(pl.multiple_of(i * NB, NB), NB)
            ncols = pl.ds(pl.multiple_of(n0 + i * NB, NB), NB)
            for m in range(ROWS // MB):
                mrows = slice(m * MB, (m + 1) * MB)
                s = lax.dot_general(
                    xb[mrows, :], pu[slot, nrows, :], (((1,), (1,)), ((), ())),
                    preferred_element_type=jnp.float32)
                epilogue(mrows, ncols, s)
            return 0

        lax.fori_loop(0, COLS // NB, body, 0)

    def kernel_block(xt, slots):
        inv = inverse_norms(xt) * (LOG2E / EPSILON)
        for g in range(ROWS // LANES):
            spread(inv[:, g * LANES:(g + 1) * LANES], inv_col, g)
        transpose_view(xt)

        def epilogue(mrows, ncols, s):
            scale = inv_col[mrows, :]
            for t in range(NB // LANES):
                part = s[:, t * LANES:(t + 1) * LANES]
                kern[mrows, pl.ds(pl.multiple_of(ncols.start + t * LANES, LANES), LANES)] = (
                    jnp.exp2(part * scale))

        for n, slot in enumerate(slots):
            products(slot, n * COLS, epilogue)

    def second_view(xt, slot):
        inv = inverse_norms(xt)
        for g in range(ROWS // LANES):
            piece = inv[:, g * LANES:(g + 1) * LANES]
            inv_row2[g:g + 1, :] = piece
            spread(piece * (LOG2E / SOFTMAX_TEMP_VALUE), inv_col, g)
        transpose_view(xt)

        def epilogue(mrows, ncols, s):
            s2[mrows, ncols] = s

        products(slot, 0, epilogue)

        def body(g, _):
            rows = pl.ds(pl.multiple_of(g * LANES, LANES), LANES)
            scale = inv_col[rows, :]
            acc = jnp.zeros((LANES, LANES), jnp.float32)
            for j in range(COLS // LANES):
                acc += jnp.exp2(s2[rows, j * LANES:(j + 1) * LANES] * scale)
            pstat[0, pl.ds(g, 1), :] = jnp.sum(jnp.transpose(acc), axis=0, keepdims=True)
            return 0

        lax.fori_loop(0, ROWS // LANES, body, 0)

    def column_pass(dst, first):
        def body(j, _):
            block = kern[:, pl.ds(pl.multiple_of(j * LANES, LANES), LANES)]
            if not first:
                block = block * col_r[...]
            part = jnp.sum(block.reshape(ROWS // 8, 8, LANES), axis=0)
            dst[pl.ds(j, 1), :] = jnp.sum(part, axis=0, keepdims=True)
            return 0

        lax.fori_loop(0, 2 * COLS // LANES, body, 0)

    def row_pass(dst):
        def body(g, _):
            rows = pl.ds(pl.multiple_of(g * LANES, LANES), LANES)
            acc = jnp.zeros((LANES, LANES), jnp.float32)
            for j in range(2 * COLS // LANES):
                acc += kern[rows, j * LANES:(j + 1) * LANES] * cvec[j:j + 1, :]
            dst[pl.ds(g, 1), :] = jnp.sum(jnp.transpose(acc), axis=0, keepdims=True)
            return 0

        lax.fori_loop(0, ROWS // LANES, body, 0)

    def cross_pass(k0, cref):
        def body(g, _):
            rows = pl.ds(pl.multiple_of(g * LANES, LANES), LANES)
            acc = jnp.zeros((LANES, LANES), jnp.float32)
            for j in range(COLS // LANES):
                acc += (
                    kern[rows, k0 + j * LANES:k0 + (j + 1) * LANES]
                    * cref[j:j + 1, :]
                    * s2[rows, j * LANES:(j + 1) * LANES])
            total = jnp.sum(jnp.transpose(acc), axis=0, keepdims=True)
            pstat[1, pl.ds(g, 1), :] = (
                total * inv_row2[pl.ds(g, 1), :] * (1.0 / SOFTMAX_TEMP_VALUE))
            return 0

        lax.fori_loop(0, ROWS // LANES, body, 0)

    def spread_rows(rows8):
        for g in range(ROWS // LANES):
            spread(rows8[g:g + 1, :], col_r, g)

    def write_out(k0, cref):
        def body(g, _):
            rows = pl.ds(pl.multiple_of(g * LANES, LANES), LANES)
            scale = col_r[rows, :] * float(TOTAL_ROWS)
            for j in range(COLS // LANES):
                lanes = slice(j * LANES, (j + 1) * LANES)
                assign = (
                    kern[rows, k0 + j * LANES:k0 + (j + 1) * LANES] * cref[j:j + 1, :]) * scale
                out_ref[rows, lanes] = (assign * float(TOTAL_PROTOS)).astype(jnp.bfloat16)
            return 0

        lax.fori_loop(0, ROWS // LANES, body, 0)

    def exchange_columns(it):
        for d in range(1, NX):
            start(colbuf.at[it, b], colbuf.at[it, b], col_rs.at[it],
                  device((b + d) % NX, y, z, c))
        peers = colbuf.at[it, pl.ds(0, NX - 1)]
        remote(peers, peers, col_rs.at[it], partner).wait_recv()
        total = (colbuf[it, 0] + colbuf[it, 1]) + (colbuf[it, 2] + colbuf[it, 3])
        cvec[...] = 1.0 / (float(TOTAL_PROTOS) * total)

    def plane_send(ref, rsem):
        for dy in range(NY):
            for dz in range(NZ):
                if dy or dz:
                    start(ref, ref, rsem, device(b, (y + dy) % NY, (z + dz) % NZ, c))

    def plane_wait(peers, rsem):
        remote(peers, peers, rsem, partner).wait_recv()

    @pl.when(c == 1)
    def _():
        own = pltpu.make_async_copy(v1_ref, xg.at[y, z, 1], local_sem.at[1])
        own.start()
        start(v2_ref, xg.at[y, z, 1], stage_sem, partner)
        normalize(1)
        own.wait()
        remote(v1_ref, xg.at[y, z, 0], stage_sem, partner).wait_recv()
        gather()
        start(xg, xp, xp_rs, partner)
        remote(pu.at[0], pu.at[0], pu_rs, partner).wait_recv()
        kernel_block(xg, (0, 1))
        for it in range(SINK_ITERS):
            column_pass(colbuf.at[it, b], it == 0)
            exchange_columns(it)
            if it == SINK_ITERS - 1:
                start(cvec.at[pl.ds(0, 8)], svec, vec_rs.at[0], partner)
            row_pass(rowbuf.at[it, chip])
            plane_send(rowbuf.at[it, chip], row_rs.at[it])
            if it == 1:
                remote(xg, xp, xp_rs, partner).wait_recv()
                second_view(xp, 1)
            if it == SINK_ITERS - 1:
                cross_pass(COLS, cvec.at[pl.ds(8, 8)])
                remote(pstat, sstat, vec_rs.at[1], partner).wait_recv()
                xbuf[chip] = pstat[...] + sstat[...]
                plane_send(xbuf.at[chip], x_rs)
            plane_wait(rowbuf.at[it, pl.ds(0, NCHIP - 1)], row_rs.at[it])
            row_sums = jnp.sum(rowbuf[it], axis=0)
            rvec[...] = 1.0 / (float(TOTAL_ROWS) * row_sums)
            if it == SINK_ITERS - 1:
                start(rvec, lvec.at[0], vec_rs.at[2], partner)
            spread_rows(rvec)
        write_out(COLS, cvec.at[pl.ds(8, 8)])
        plane_wait(xbuf.at[pl.ds(0, NCHIP - 1)], x_rs)
        stats = jnp.sum(xbuf[...], axis=0)
        row_sums = jnp.sum(rowbuf[SINK_ITERS - 1], axis=0)
        loss = jnp.log(stats[0]) - stats[1] / row_sums
        loss_ref[...] = loss
        lvec[1] = loss
        start(lvec.at[1], lvec.at[1], vec_rs.at[3], partner)
        drain()

    @pl.when(c == 0)
    def _():
        own = pltpu.make_async_copy(v2_ref, xg.at[y, z, 0], local_sem.at[1])
        own.start()
        start(v1_ref, xg.at[y, z, 0], stage_sem, partner)
        normalize(0)
        start(pu.at[0], pu.at[0], pu_rs, partner)
        own.wait()
        remote(v2_ref, xg.at[y, z, 1], stage_sem, partner).wait_recv()
        remote(xg, xp, xp_rs, partner).wait_recv()
        gather()
        start(xg, xp, xp_rs, partner)
        kernel_block(xp, (0,))
        second_view(xg, 0)
        remote(cvec.at[pl.ds(0, 8)], svec, vec_rs.at[0], partner).wait_recv()
        cross_pass(0, svec)
        start(pstat, sstat, vec_rs.at[1], partner)
        remote(rvec, lvec.at[0], vec_rs.at[2], partner).wait_recv()
        spread_rows(lvec.at[0])
        write_out(0, svec)
        remote(lvec.at[1], lvec.at[1], vec_rs.at[3], partner).wait_recv()
        loss_ref[...] = lvec[1]
        drain()


def local(view_codes, predictor_view_embeddings, prototypes):
    f32, bf16 = jnp.float32, jnp.bfloat16
    anywhere = pl.BlockSpec(memory_space=pl.ANY)
    vmem = pl.BlockSpec(memory_space=pltpu.VMEM)
    dma = pltpu.SemaphoreType.DMA
    assignments, loss = pl.pallas_call(
        swap_kernel,
        out_shape=(
            jax.ShapeDtypeStruct((ROWS, COLS), bf16),
            jax.ShapeDtypeStruct((8, LANES), f32),
        ),
        in_specs=[anywhere] * 3,
        out_specs=(vmem, vmem),
        scratch_shapes=[
            pltpu.VMEM((NY, NZ, 2, SHARD, ROWS), bf16),
            pltpu.VMEM((NY, NZ, 2, SHARD, ROWS), bf16),
            pltpu.VMEM((COLS, DIM), bf16),
            pltpu.VMEM((2, COLS, DIM), bf16),
            pltpu.VMEM((ROWS, 2 * COLS), f32),
            pltpu.VMEM((ROWS, COLS), f32),
            pltpu.VMEM((ROWS, DIM), bf16),
            pltpu.VMEM((ROWS, LANES), f32),
            pltpu.VMEM((ROWS, LANES), f32),
            pltpu.VMEM((SINK_ITERS, NX, 16, LANES), f32),
            pltpu.VMEM((SINK_ITERS, NCHIP, 8, LANES), f32),
            pltpu.VMEM((NCHIP, 2, 8, LANES), f32),
            pltpu.VMEM((16, LANES), f32),
            pltpu.VMEM((8, LANES), f32),
            pltpu.VMEM((8, LANES), f32),
            pltpu.VMEM((2, 8, LANES), f32),
            pltpu.VMEM((2, 8, LANES), f32),
            pltpu.VMEM((2, 8, LANES), f32),
            pltpu.VMEM((8, LANES), f32),
            dma((2,)),
            dma(()),
            dma((NY, NZ, 2)),
            dma(()),
            dma(()),
            dma(()),
            dma((SINK_ITERS,)),
            dma((SINK_ITERS,)),
            dma(()),
            dma((4,)),
        ],
        compiler_params=pltpu.CompilerParams(
            collective_id=0, has_side_effects=True, vmem_limit_bytes=48 << 20),
        name="swapped_sinkhorn",
    )(view_codes.T, predictor_view_embeddings.T, prototypes)
    return assignments, loss.reshape(ROWS)


def solution(mesh):
    placed = (P("batch", "proto"), P("batch", "proto"), P("proto", None))
    return jax.shard_map(
        local,
        mesh=mesh,
        in_specs=placed,
        out_specs=(P("batch", "proto"), P("batch")),
        check_vma=False,
    )
```

```python
import functools
import math

import jax
import jax.numpy as jnp
from jax import lax
from jax.experimental import pallas as pl
from jax.experimental.pallas import tpu as pltpu
from jax.sharding import PartitionSpec as P

SINK_ITERS = 3
EPSILON = 0.05
SOFTMAX_TEMP_VALUE = 0.1
LOG2E = math.log2(math.e)

MESH = pl.DeviceIdType.MESH
NX, NY, NZ = 4, 4, 8
NCHIP = NY * NZ
ROWS = 1024
COLS = 1024
DIM = 1024
SHARD = 16
LANES = 128
TOTAL_ROWS = 4096
TOTAL_PROTOS = 65536
GO_STEP = 0


def swap_kernel(
    v1_ref, v2_ref, p_ref, out_ref, loss_ref,
    xg, xp, praw, pt, kern, s2, xb, vstage, squares, rscr, col_r, inv_col,
    colbuf, rowbuf, tbuf, xbuf, cvec, svec, rvec, lvec, sstat, pstat, inv_row2,
    local_sem, stage_sem, gather_rs, send_sem, xp_rs, pu_rs, col_rs, row_rs, t_rs, x_rs, vec_rs, go_sem,
):
    b = lax.axis_index("batch")
    q = lax.axis_index("proto")
    c = q % 2
    z = (q // 2) % NZ
    y = q // (2 * NZ)
    chip = y * NZ + z

    def device(bb, yy, zz, cc):
        return (bb, yy * (2 * NZ) + zz * 2 + cc)

    def at_y(d):
        return device(b, (y + d) % NY, z, c)

    def at_z(d):
        return device(b, y, (z + d) % NZ, c)

    partner = device(b, y, z, 1 - c)
    sent = []

    def remote(src, dst, rsem, dev):
        return pltpu.make_async_remote_copy(
            src_ref=src, dst_ref=dst, send_sem=send_sem, recv_sem=rsem,
            device_id=dev, device_id_type=MESH)

    def start(src, dst, rsem, dev):
        copy = remote(src, dst, rsem, dev)
        copy.start()
        sent.append(copy)

    def drain():
        for copy in sent:
            copy.wait_send()
        sent.clear()

    own_p = pltpu.make_async_copy(p_ref, praw, local_sem.at[0])
    own_p.start()

    def load(src, dst, sem):
        copy = pltpu.make_async_copy(src, dst, sem)
        copy.start()
        return copy

    barrier = pltpu.get_barrier_semaphore()
    greet = [partner]
    greet += [device((b + d) % NX, y, z, c) for d in range(1, NX)]
    greet += [at_y(d) for d in range(1, NY)]
    greet += [at_z(d) for d in range(1, NZ)]
    for dev in greet:
        pl.semaphore_signal(barrier, 1, device_id=dev, device_id_type=MESH)

    def enter():
        pl.semaphore_wait(barrier, len(greet))

    def normalize(slot):
        own_p.wait()

        def body(i, _):
            rows = pl.ds(pl.multiple_of(i * LANES, LANES), LANES)
            w = praw[rows, :].astype(jnp.float32)
            total = jnp.sum(w * w, axis=1, keepdims=True)
            unit = (w * lax.rsqrt(total + 1e-06)).astype(jnp.bfloat16)
            pt[slot, :, :, :, rows] = jnp.transpose(unit).reshape(NY, NZ, 2 * SHARD, LANES)
            return 0

        lax.fori_loop(0, COLS // LANES, body, 0)

    def put(yy, zz, h, dev):
        start(xg.at[yy, zz, h], xg.at[yy, zz, h], gather_rs.at[yy, zz, h], dev)

    def arrived(yy, zz, h):
        remote(xg.at[yy, zz, h], xg.at[yy, zz, h], gather_rs.at[yy, zz, h], partner).wait_recv()

    def hops(j, direction):
        far = NZ // 2
        if direction > 0:
            return far if j in (0, 1) else far - 1
        return far - 1 if j in (0, 1) else far

    def gather(own_half, work):
        def yj(j):
            return (y + j) % NY

        def zk(k):
            return (z + k) % NZ

        def first_puts(h):
            put(y, z, h, at_z(1))
            put(y, z, h, at_z(NZ - 1))
            for d in (2, 1, 3):
                put(y, z, h, at_y(d))

        own_half(first_puts)

        def ring(k, js):
            for direction in (1, -1):
                zz = zk(NZ - k) if direction > 0 else zk(k)
                nxt = at_z(1) if direction > 0 else at_z(NZ - 1)
                for j in js:
                    if hops(j, direction) >= k:
                        arrived(yj(j), zz, 0)
                        if hops(j, direction) > k:
                            put(yj(j), zz, 0, nxt)
                    if j == 0 and hops(1, direction) >= k:
                        arrived(y, zz, 1)
                        if hops(1, direction) > k:
                            put(y, zz, 1, nxt)
                        for d in (2, 1, 3):
                            put(y, zz, 1, at_y(d))

        far = NZ // 2
        ring(1, (0,))
        for j in (1, 3, 2):
            arrived(yj(j), z, 0)
            put(yj(j), z, 0, at_z(1))
            put(yj(j), z, 0, at_z(NZ - 1))
        for k in range(1, far + 1):
            if k < far:
                ring(k + 1, (0,))
            ring(k, (1, 3, 2))
            offsets = (k, NZ - k) if k < far else (0, far)
            if k > 1:
                work(2 * k - 3)
            for o in offsets:
                for j in (1, 3, 2):
                    arrived(yj(j), zk(o), 1)
            work(2 * k - 2, zk(offsets[0]), zk(offsets[1]))

    def row_squares(block):
        v = block.astype(jnp.float32)
        return jnp.sum((v * v).reshape(-1, 8, ROWS), axis=0)

    def spread(row, dst, g):
        dst[g * LANES:(g + 1) * LANES, :] = jnp.transpose(
            jnp.broadcast_to(row, (LANES, LANES)))

    def spread_scale(inv, factor):
        for g in range(ROWS // LANES):
            spread(inv[:, g * LANES:(g + 1) * LANES] * factor, inv_col, g)

    def inverse(sums):
        return lax.rsqrt(jnp.sum(sums, axis=0, keepdims=True) + 1e-06)

    def transpose_view(xt):
        sums = jnp.zeros((8, ROWS), jnp.float32)
        for kb in range(DIM // LANES):
            yy, z0 = kb // 2, (kb % 2) * 4
            block = xt[yy, z0:z0 + 4].reshape(LANES, ROWS)
            xb[:, kb * LANES:(kb + 1) * LANES] = jnp.transpose(block)
            sums += row_squares(block)
        return inverse(sums)

    NB = 256

    def chunk_load(k, z0, z1):
        sums = jnp.zeros((8, ROWS), jnp.float32)
        for i, zz in enumerate((z0, z1)):
            block = xg[:, zz].reshape(LANES, ROWS)
            at = (k - 1) * 2 * LANES + i * LANES
            xb[:, at:at + LANES] = jnp.transpose(block)
            sums += row_squares(block)
        if k > 1:
            sums += squares[...]
        squares[...] = sums
        if k == NZ // 2:
            spread_scale(inverse(sums), LOG2E / EPSILON)

    def chunk_product(k, z0, z1, slot):
        first, last = k == 1, k == NZ // 2
        depth = slice((k - 1) * 2 * LANES, k * 2 * LANES)
        for t in range(COLS // NB):
            lanes = slice(t * NB, (t + 1) * NB)
            rhs = jnp.concatenate([
                pt[slot, :, zz, :, lanes].reshape(LANES, NB) for zz in (z0, z1)], axis=0)
            cols = slice(slot * COLS + t * NB, slot * COLS + (t + 1) * NB)
            part = jnp.zeros((8, NB), jnp.float32)
            for m in range(ROWS // NB):
                mrows = slice(m * NB, (m + 1) * NB)
                s = jnp.dot(xb[mrows, depth], rhs, preferred_element_type=jnp.float32)
                if not first:
                    s = s + kern[mrows, cols]
                if last:
                    scale = inv_col[mrows, :]
                    s = jnp.exp2(s * jnp.concatenate([scale, scale], axis=1))
                    part += jnp.sum(s.reshape(NB // 8, 8, NB), axis=0)
                kern[mrows, cols] = s
            if last:
                total = jnp.sum(part, axis=0, keepdims=True)
                for u in range(NB // LANES):
                    row = slot * (COLS // LANES) + t * (NB // LANES) + u
                    colbuf[0, b, row:row + 1, :] = total[:, u * LANES:(u + 1) * LANES]

    MB = 512

    def products(slot, epilogue):
        def body(i, _):
            ncols = pl.ds(pl.multiple_of(i * NB, NB), NB)
            rhs = pt[slot, :, :, :, ncols].reshape(DIM, NB)
            for m in range(ROWS // MB):
                mrows = slice(m * MB, (m + 1) * MB)
                s = jnp.dot(xb[mrows, :], rhs, preferred_element_type=jnp.float32)
                epilogue(mrows, ncols, s)
            return 0

        lax.fori_loop(0, COLS // NB, body, 0)

    def kernel_block(xt, slot):
        spread_scale(transpose_view(xt), LOG2E / EPSILON)

        def epilogue(mrows, ncols, s):
            scale = inv_col[mrows, :]
            kern[mrows, ncols] = jnp.exp2(s * jnp.concatenate([scale, scale], axis=1))

        products(slot, epilogue)

    def gather_lanes(dst):
        for g in range(ROWS // LANES):
            dst[g:g + 1, :] = jnp.sum(
                jnp.transpose(rscr[g * LANES:(g + 1) * LANES, :]), axis=0, keepdims=True)

    def second_view(xt, slot):
        inv = transpose_view(xt)
        for g in range(ROWS // LANES):
            inv_row2[g:g + 1, :] = inv[:, g * LANES:(g + 1) * LANES]
        spread_scale(inv, LOG2E / SOFTMAX_TEMP_VALUE)
        rscr[...] = jnp.zeros((ROWS, LANES), jnp.float32)

        def epilogue(mrows, ncols, s):
            s2[mrows, ncols] = s
            scale = inv_col[mrows, :]
            e = jnp.exp2(s * jnp.concatenate([scale, scale], axis=1))
            rscr[mrows, :] += e[:, :LANES] + e[:, LANES:]

        products(slot, epilogue)
        gather_lanes(pstat.at[0])

    def column_pass(dst):
        nj = 2 * COLS // LANES

        def body(g, accs):
            rows = pl.ds(pl.multiple_of(g * 8, 8), 8)
            r = col_r[rows, :]
            return tuple(
                acc + kern[rows, j * LANES:(j + 1) * LANES] * r for j, acc in enumerate(accs))

        zero = jnp.zeros((8, LANES), jnp.float32)
        accs = lax.fori_loop(0, ROWS // 8, body, (zero,) * nj, unroll=4)
        for j in range(nj):
            dst[j:j + 1, :] = jnp.sum(accs[j], axis=0, keepdims=True)

    def row_pass(dst):
        nj = 2 * COLS // LANES

        def body(g, _):
            rows = pl.ds(pl.multiple_of(g * 64, 64), 64)
            acc = jnp.zeros((64, LANES), jnp.float32)
            for j in range(nj):
                acc += kern[rows, j * LANES:(j + 1) * LANES] * cvec[j:j + 1, :]
            rscr[rows, :] = acc
            return 0

        lax.fori_loop(0, ROWS // 64, body, 0, unroll=2)
        gather_lanes(dst)

    def cross_pass(k0, cref):
        def body(g, _):
            rows = pl.ds(pl.multiple_of(g * 64, 64), 64)
            acc = jnp.zeros((64, LANES), jnp.float32)
            for j in range(COLS // LANES):
                acc += (
                    kern[rows, k0 + j * LANES:k0 + (j + 1) * LANES]
                    * cref[j:j + 1, :]
                    * s2[rows, j * LANES:(j + 1) * LANES])
            rscr[rows, :] = acc
            return 0

        lax.fori_loop(0, ROWS // 64, body, 0, unroll=2)
        gather_lanes(pstat.at[1])
        pstat[1] = pstat[1] * inv_row2[...] * (1.0 / SOFTMAX_TEMP_VALUE)

    def spread_rows(rows8):
        for g in range(ROWS // LANES):
            spread(rows8[g:g + 1, :], col_r, g)

    def write_out(k0, cref):
        def body(g, _):
            rows = pl.ds(pl.multiple_of(g * LANES, LANES), LANES)
            scale = col_r[rows, :] * float(TOTAL_ROWS)
            for j in range(COLS // LANES):
                lanes = slice(j * LANES, (j + 1) * LANES)
                assign = (
                    kern[rows, k0 + j * LANES:k0 + (j + 1) * LANES] * cref[j:j + 1, :]) * scale
                out_ref[rows, lanes] = (assign * float(TOTAL_PROTOS)).astype(jnp.bfloat16)
            return 0

        lax.fori_loop(0, ROWS // LANES, body, 0)

    def exchange_columns(it):
        for d in range(1, NX):
            start(colbuf.at[it, b], colbuf.at[it, b], col_rs.at[it],
                  device((b + d) % NX, y, z, c))
        peers = colbuf.at[it, pl.ds(0, NX - 1)]
        remote(peers, peers, col_rs.at[it], partner).wait_recv()
        total = (colbuf[it, 0] + colbuf[it, 1]) + (colbuf[it, 2] + colbuf[it, 3])
        cvec[...] = 1.0 / (float(TOTAL_PROTOS) * total)

    def plane_send(ref, rsem):
        offsets = [(dy, dz) for dy in range(NY) for dz in range(NZ) if dy or dz]
        offsets.sort(key=lambda o: -(min(o[0], NY - o[0]) + min(o[1], NZ - o[1])))
        for dy, dz in offsets:
            start(ref, ref, rsem, device(b, (y + dy) % NY, (z + dz) % NZ, c))

    def plane_wait(peers, rsem):
        remote(peers, peers, rsem, partner).wait_recv()

    def share(zs):
        for zz in zs:
            start(xg.at[:, zz], xp.at[:, zz], xp_rs, partner)

    @pl.when(c == 1)
    def _():
        own = load(v1_ref, xg.at[y, z, 1], local_sem.at[1])
        other = load(v2_ref, vstage, local_sem.at[2])
        normalize(1)
        own.wait()
        other.wait()
        enter()
        start(vstage, xg.at[y, z, 1], stage_sem, partner)

        def own_half(first_puts):
            first_puts(1)
            remote(vstage, xg.at[y, z, 0], stage_sem, partner).wait_recv()
            first_puts(0)

        loaded = []

        def work(step, *zs):
            k = step // 2 + 1
            if zs:
                loaded.append(zs)
                share(zs)
                chunk_load(k, *zs)
            if step % 2 == 0:
                chunk_product(k, *loaded[k - 1], 1)
            if step == GO_STEP:
                pl.semaphore_signal(go_sem, 1, device_id=partner, device_id_type=MESH)
            if step == 1:
                remote(pt.at[0], pt.at[0], pu_rs, partner).wait_recv()
            if step % 2 == 1 or k == NZ // 2:
                chunk_product(k, *loaded[k - 1], 0)

        gather(own_half, work)
        for it in range(SINK_ITERS):
            if it > 0:
                column_pass(colbuf.at[it, b])
            exchange_columns(it)
            if it == SINK_ITERS - 1:
                start(cvec.at[pl.ds(0, 8)], svec, vec_rs.at[0], partner)
            row_pass(rowbuf.at[it, chip])
            plane_send(rowbuf.at[it, chip], row_rs.at[it])
            if it == 1:
                remote(xg, xp, xp_rs, partner).wait_recv()
                second_view(xp, 1)
                remote(pstat.at[0], sstat.at[0], vec_rs.at[4], partner).wait_recv()
                tbuf[chip] = pstat[0] + sstat[0]
                plane_send(tbuf.at[chip], t_rs)
            if it == SINK_ITERS - 1:
                cross_pass(COLS, cvec.at[pl.ds(8, 8)])
                remote(pstat.at[1], sstat.at[1], vec_rs.at[1], partner).wait_recv()
                xbuf[chip] = pstat[1] + sstat[1]
                plane_send(xbuf.at[chip], x_rs)
            plane_wait(rowbuf.at[it, pl.ds(0, NCHIP - 1)], row_rs.at[it])
            row_sums = jnp.sum(rowbuf[it], axis=0)
            rvec[...] = 1.0 / (float(TOTAL_ROWS) * row_sums)
            if it == SINK_ITERS - 1:
                start(rvec, lvec.at[0], vec_rs.at[2], partner)
            spread_rows(rvec)
        write_out(COLS, cvec.at[pl.ds(8, 8)])
        plane_wait(tbuf.at[pl.ds(0, NCHIP - 1)], t_rs)
        totals = jnp.log(jnp.sum(tbuf[...], axis=0))
        row_sums = jnp.sum(rowbuf[SINK_ITERS - 1], axis=0)
        plane_wait(xbuf.at[pl.ds(0, NCHIP - 1)], x_rs)
        loss = totals - jnp.sum(xbuf[...], axis=0) / row_sums
        loss_ref[...] = loss
        lvec[1] = loss
        start(lvec.at[1], lvec.at[1], vec_rs.at[3], partner)
        drain()

    @pl.when(c == 0)
    def _():
        own = load(v2_ref, xg.at[y, z, 0], local_sem.at[1])
        other = load(v1_ref, vstage, local_sem.at[2])
        normalize(0)
        own.wait()
        other.wait()
        enter()
        start(vstage, xg.at[y, z, 0], stage_sem, partner)
        start(pt.at[0], pt.at[0], pu_rs, partner)

        def own_half(first_puts):
            first_puts(0)
            remote(vstage, xg.at[y, z, 1], stage_sem, partner).wait_recv()
            first_puts(1)

        def work(step, *zs):
            share(zs)

        pl.semaphore_wait(go_sem, 1)
        gather(own_half, work)
        second_view(xg, 0)
        start(pstat.at[0], sstat.at[0], vec_rs.at[4], partner)
        remote(xg, xp, xp_rs, partner).wait_recv()
        kernel_block(xp, 0)
        remote(cvec.at[pl.ds(0, 8)], svec, vec_rs.at[0], partner).wait_recv()
        cross_pass(0, svec)
        start(pstat.at[1], sstat.at[1], vec_rs.at[1], partner)
        remote(rvec, lvec.at[0], vec_rs.at[2], partner).wait_recv()
        spread_rows(lvec.at[0])
        write_out(0, svec)
        remote(lvec.at[1], lvec.at[1], vec_rs.at[3], partner).wait_recv()
        loss_ref[...] = lvec[1]
        drain()


def local(view_codes, predictor_view_embeddings, prototypes):
    f32, bf16 = jnp.float32, jnp.bfloat16
    anywhere = pl.BlockSpec(memory_space=pltpu.HBM)
    vmem = pl.BlockSpec(memory_space=pltpu.VMEM)
    dma = pltpu.SemaphoreType.DMA
    assignments, loss = pl.pallas_call(
        swap_kernel,
        out_shape=(
            jax.ShapeDtypeStruct((ROWS, COLS), bf16),
            jax.ShapeDtypeStruct((8, LANES), f32),
        ),
        in_specs=[anywhere] * 3,
        out_specs=(vmem, vmem),
        scratch_shapes=[
            pltpu.VMEM((NY, NZ, 2, SHARD, ROWS), bf16),
            pltpu.VMEM((NY, NZ, 2, SHARD, ROWS), bf16),
            pltpu.VMEM((COLS, DIM), bf16),
            pltpu.VMEM((2, NY, NZ, 2 * SHARD, COLS), bf16),
            pltpu.VMEM((ROWS, 2 * COLS), f32),
            pltpu.VMEM((ROWS, COLS), f32),
            pltpu.VMEM((ROWS, DIM), bf16),
            pltpu.VMEM((SHARD, ROWS), bf16),
            pltpu.VMEM((8, ROWS), f32),
            pltpu.VMEM((ROWS, LANES), f32),
            pltpu.VMEM((ROWS, LANES), f32),
            pltpu.VMEM((ROWS, LANES), f32),
            pltpu.VMEM((SINK_ITERS, NX, 16, LANES), f32),
            pltpu.VMEM((SINK_ITERS, NCHIP, 8, LANES), f32),
            pltpu.VMEM((NCHIP, 8, LANES), f32),
            pltpu.VMEM((NCHIP, 8, LANES), f32),
            pltpu.VMEM((16, LANES), f32),
            pltpu.VMEM((8, LANES), f32),
            pltpu.VMEM((8, LANES), f32),
            pltpu.VMEM((2, 8, LANES), f32),
            pltpu.VMEM((2, 8, LANES), f32),
            pltpu.VMEM((2, 8, LANES), f32),
            pltpu.VMEM((8, LANES), f32),
            dma((3,)),
            dma(()),
            dma((NY, NZ, 2)),
            dma(()),
            dma(()),
            dma(()),
            dma((SINK_ITERS,)),
            dma((SINK_ITERS,)),
            dma(()),
            dma(()),
            dma((5,)),
            pltpu.SemaphoreType.REGULAR,
        ],
        compiler_params=pltpu.CompilerParams(
            collective_id=0, has_side_effects=True, vmem_limit_bytes=48 << 20),
        name="swapped_sinkhorn",
    )(*[pltpu.with_memory_space_constraint(a, pltpu.HBM) for a in (
        view_codes.T, predictor_view_embeddings.T, prototypes)])
    return assignments, loss.reshape(ROWS)


def solution(mesh):
    placed = (P("batch", "proto"), P("batch", "proto"), P("proto", None))
    return jax.shard_map(
        local,
        mesh=mesh,
        in_specs=placed,
        out_specs=(P("batch", "proto"), P("batch")),
        check_vma=False,
    )
```

```python
import functools
import math

import jax
import jax.numpy as jnp
from jax import lax
from jax.experimental import pallas as pl
from jax.experimental.pallas import tpu as pltpu
from jax.sharding import PartitionSpec as P

SINK_ITERS = 3
EPSILON = 0.05
SOFTMAX_TEMP_VALUE = 0.1
LOG2E = math.log2(math.e)

MESH = pl.DeviceIdType.MESH
NX, NY, NZ = 4, 4, 8
NCHIP = NY * NZ
ROWS = 1024
COLS = 1024
DIM = 1024
SHARD = 16
LANES = 128
TOTAL_ROWS = 4096
TOTAL_PROTOS = 65536


def swap_kernel(
    v1_ref, v2_ref, p_ref, out_ref, loss_ref,
    xg, xp, praw, pt, kern, s2, xb, vstage, squares, rscr, col_r, inv_col,
    colbuf, rowbuf, tbuf, xbuf, cvec, svec, rvec, lvec, sstat, pstat, inv_row2,
    local_sem, gather_rs, send_sem, xp_rs, pu_rs, col_rs, row_rs, t_rs, x_rs, vec_rs, go_sem,
):
    b = lax.axis_index("batch")
    q = lax.axis_index("proto")
    c = q % 2
    z = (q // 2) % NZ
    y = q // (2 * NZ)
    chip = y * NZ + z

    def device(bb, yy, zz, cc):
        return (bb, yy * (2 * NZ) + zz * 2 + cc)

    def at_y(d):
        return device(b, (y + d) % NY, z, c)

    def at_z(d):
        return device(b, y, (z + d) % NZ, c)

    partner = device(b, y, z, 1 - c)
    sent = []

    def remote(src, dst, rsem, dev):
        return pltpu.make_async_remote_copy(
            src_ref=src, dst_ref=dst, send_sem=send_sem, recv_sem=rsem,
            device_id=dev, device_id_type=MESH)

    def start(src, dst, rsem, dev):
        copy = remote(src, dst, rsem, dev)
        copy.start()
        sent.append(copy)

    def drain():
        for copy in sent:
            copy.wait_send()
        sent.clear()

    own_p = pltpu.make_async_copy(p_ref, praw, local_sem.at[0])
    own_p.start()

    def load(src, dst, sem):
        copy = pltpu.make_async_copy(src, dst, sem)
        copy.start()
        return copy

    barrier = pltpu.get_barrier_semaphore()
    greet = [partner]
    greet += [device((b + d) % NX, y, z, c) for d in range(1, NX)]
    near = [(d, 0) for d in (2, 1, 3)] + [(0, 1), (0, NZ - 1)]
    for cc in (c, 1 - c):
        greet += [device(b, (y + dy) % NY, (z + dz) % NZ, cc) for dy, dz in near]
    for dev in greet:
        pl.semaphore_signal(barrier, 1, device_id=dev, device_id_type=MESH)

    def enter():
        pl.semaphore_wait(barrier, len(greet))

    def normalize(slot):
        own_p.wait()

        def body(i, _):
            rows = pl.ds(pl.multiple_of(i * LANES, LANES), LANES)
            w = praw[rows, :].astype(jnp.float32)
            total = jnp.sum(w * w, axis=1, keepdims=True)
            unit = (w * lax.rsqrt(total + 1e-06)).astype(jnp.bfloat16)
            pt[slot, :, :, :, rows] = jnp.transpose(unit).reshape(NY, NZ, 2 * SHARD, LANES)
            return 0

        lax.fori_loop(0, COLS // LANES, body, 0)

    def put(yy, zz, h, dev):
        start(xg.at[yy, zz, h], xg.at[yy, zz, h], gather_rs.at[yy, zz, h], dev)

    def arrived(yy, zz, h):
        remote(xg.at[yy, zz, h], xg.at[yy, zz, h], gather_rs.at[yy, zz, h], partner).wait_recv()

    def hops(j, direction):
        far = NZ // 2
        if direction > 0:
            return far if j in (0, 1) else far - 1
        return far - 1 if j in (0, 1) else far

    def hand_over(h):
        opposite = 1 - c
        rsem = gather_rs.at[y, z, h]
        for dy, dz in ((0, 1), (0, NZ - 1), (2, 0), (1, 0), (3, 0)):
            start(vstage, xg.at[y, z, h], rsem,
                  device(b, (y + dy) % NY, (z + dz) % NZ, opposite))
        start(vstage, xg.at[y, z, h], rsem, partner)

    def gather(own, work):
        def yj(j):
            return (y + j) % NY

        def zk(k):
            return (z + k) % NZ

        put(y, z, own, at_z(1))
        put(y, z, own, at_z(NZ - 1))
        for d in (2, 1, 3):
            put(y, z, own, at_y(d))

        def ring(k, js):
            for direction in (1, -1):
                zz = zk(NZ - k) if direction > 0 else zk(k)
                nxt = at_z(1) if direction > 0 else at_z(NZ - 1)
                for j in js:
                    if hops(j, direction) >= k:
                        arrived(yj(j), zz, 0)
                        if hops(j, direction) > k:
                            put(yj(j), zz, 0, nxt)
                    if j == 0 and hops(1, direction) >= k:
                        arrived(y, zz, 1)
                        if hops(1, direction) > k:
                            put(y, zz, 1, nxt)
                        for d in (2, 1, 3):
                            put(y, zz, 1, at_y(d))

        far = NZ // 2
        ring(1, (0,))
        for j in (1, 3, 2):
            arrived(yj(j), z, 0)
            put(yj(j), z, 0, at_z(1))
            put(yj(j), z, 0, at_z(NZ - 1))
        for k in range(1, far + 1):
            if k < far:
                ring(k + 1, (0,))
                if k > 1:
                    work(k - 1)
            ring(k, (1, 3, 2))
            offsets = (k, NZ - k) if k < far else (0, far)
            for o in offsets:
                for j in (1, 3, 2):
                    arrived(yj(j), zk(o), 1)
            if k == far:
                arrived(y, z, 1 - own)
            work(k, zk(offsets[0]), zk(offsets[1]))

    def row_squares(block):
        v = block.astype(jnp.float32)
        return jnp.sum((v * v).reshape(-1, 8, ROWS), axis=0)

    def spread(row, dst, g):
        dst[g * LANES:(g + 1) * LANES, :] = jnp.transpose(
            jnp.broadcast_to(row, (LANES, LANES)))

    def spread_scale(inv, factor):
        for g in range(ROWS // LANES):
            spread(inv[:, g * LANES:(g + 1) * LANES] * factor, inv_col, g)

    def inverse(sums):
        return lax.rsqrt(jnp.sum(sums, axis=0, keepdims=True) + 1e-06)

    def transpose_view(xt):
        sums = jnp.zeros((8, ROWS), jnp.float32)
        for kb in range(DIM // LANES):
            yy, z0 = kb // 2, (kb % 2) * 4
            block = xt[yy, z0:z0 + 4].reshape(LANES, ROWS)
            xb[:, kb * LANES:(kb + 1) * LANES] = jnp.transpose(block)
            sums += row_squares(block)
        return inverse(sums)

    NB = 256

    def chunk_load(k, z0, z1):
        sums = jnp.zeros((8, ROWS), jnp.float32)
        for i, zz in enumerate((z0, z1)):
            block = xg[:, zz].reshape(LANES, ROWS)
            at = (k - 1) * 2 * LANES + i * LANES
            xb[:, at:at + LANES] = jnp.transpose(block)
            sums += row_squares(block)
        if k > 1:
            sums += squares[...]
        squares[...] = sums
        if k == NZ // 2:
            spread_scale(inverse(sums), LOG2E / EPSILON)

    def chunk_product(k, z0, z1, slot):
        first, last = k == 1, k == NZ // 2
        depth = slice((k - 1) * 2 * LANES, k * 2 * LANES)
        for t in range(COLS // NB):
            lanes = slice(t * NB, (t + 1) * NB)
            rhs = jnp.concatenate([
                pt[slot, :, zz, :, lanes].reshape(LANES, NB) for zz in (z0, z1)], axis=0)
            cols = slice(slot * COLS + t * NB, slot * COLS + (t + 1) * NB)
            part = jnp.zeros((8, NB), jnp.float32)
            for m in range(ROWS // NB):
                mrows = slice(m * NB, (m + 1) * NB)
                s = jnp.dot(xb[mrows, depth], rhs, preferred_element_type=jnp.float32)
                if not first:
                    s = s + kern[mrows, cols]
                if last:
                    scale = inv_col[mrows, :]
                    s = jnp.exp2(s * jnp.concatenate([scale, scale], axis=1))
                    part += jnp.sum(s.reshape(NB // 8, 8, NB), axis=0)
                kern[mrows, cols] = s
            if last:
                total = jnp.sum(part, axis=0, keepdims=True)
                for u in range(NB // LANES):
                    row = slot * (COLS // LANES) + t * (NB // LANES) + u
                    colbuf[0, b, row:row + 1, :] = total[:, u * LANES:(u + 1) * LANES]

    MB = 512

    def products(slot, epilogue):
        def body(i, _):
            ncols = pl.ds(pl.multiple_of(i * NB, NB), NB)
            rhs = pt[slot, :, :, :, ncols].reshape(DIM, NB)
            for m in range(ROWS // MB):
                mrows = slice(m * MB, (m + 1) * MB)
                s = jnp.dot(xb[mrows, :], rhs, preferred_element_type=jnp.float32)
                epilogue(mrows, ncols, s)
            return 0

        lax.fori_loop(0, COLS // NB, body, 0)

    def kernel_block(xt, slot):
        spread_scale(transpose_view(xt), LOG2E / EPSILON)

        def epilogue(mrows, ncols, s):
            scale = inv_col[mrows, :]
            value = jnp.exp2(s * jnp.concatenate([scale, scale], axis=1))
            kern[mrows, ncols] = value
            s2[mrows, ncols] = s2[mrows, ncols] * value

        products(slot, epilogue)

    def gather_lanes(dst):
        for g in range(ROWS // LANES):
            dst[g:g + 1, :] = jnp.sum(
                jnp.transpose(rscr[g * LANES:(g + 1) * LANES, :]), axis=0, keepdims=True)

    def second_view(xt, slot):
        inv = transpose_view(xt)
        for g in range(ROWS // LANES):
            inv_row2[g:g + 1, :] = inv[:, g * LANES:(g + 1) * LANES]
        spread_scale(inv, LOG2E / SOFTMAX_TEMP_VALUE)
        rscr[...] = jnp.zeros((ROWS, LANES), jnp.float32)

        def epilogue(mrows, ncols, s):
            s2[mrows, ncols] = s
            scale = inv_col[mrows, :]
            e = jnp.exp2(s * jnp.concatenate([scale, scale], axis=1))
            rscr[mrows, :] += e[:, :LANES] + e[:, LANES:]

        products(slot, epilogue)
        gather_lanes(pstat.at[0])

    def column_pass(dst):
        nj = 2 * COLS // LANES

        def body(g, accs):
            rows = pl.ds(pl.multiple_of(g * 8, 8), 8)
            r = col_r[rows, :]
            return tuple(
                acc + kern[rows, j * LANES:(j + 1) * LANES] * r for j, acc in enumerate(accs))

        zero = jnp.zeros((8, LANES), jnp.float32)
        accs = lax.fori_loop(0, ROWS // 8, body, (zero,) * nj, unroll=4)
        for j in range(nj):
            dst[j:j + 1, :] = jnp.sum(accs[j], axis=0, keepdims=True)

    def row_pass(dst):
        nj = 2 * COLS // LANES

        def body(g, _):
            rows = pl.ds(pl.multiple_of(g * 64, 64), 64)
            acc = jnp.zeros((64, LANES), jnp.float32)
            for j in range(nj):
                acc += kern[rows, j * LANES:(j + 1) * LANES] * cvec[j:j + 1, :]
            rscr[rows, :] = acc
            return 0

        lax.fori_loop(0, ROWS // 64, body, 0, unroll=2)
        gather_lanes(dst)

    def cross_pass(k0, cref, ready):
        def body(g, _):
            rows = pl.ds(pl.multiple_of(g * 64, 64), 64)
            acc = jnp.zeros((64, LANES), jnp.float32)
            for j in range(COLS // LANES):
                term = s2[rows, j * LANES:(j + 1) * LANES] * cref[j:j + 1, :]
                if not ready:
                    term = term * kern[rows, k0 + j * LANES:k0 + (j + 1) * LANES]
                acc += term
            rscr[rows, :] = acc
            return 0

        lax.fori_loop(0, ROWS // 64, body, 0, unroll=2)
        gather_lanes(pstat.at[1])
        pstat[1] = pstat[1] * inv_row2[...] * (1.0 / SOFTMAX_TEMP_VALUE)

    def spread_rows(rows8):
        for g in range(ROWS // LANES):
            spread(rows8[g:g + 1, :], col_r, g)

    def write_out(k0, cref):
        def body(g, _):
            rows = pl.ds(pl.multiple_of(g * LANES, LANES), LANES)
            scale = col_r[rows, :] * float(TOTAL_ROWS)
            for j in range(COLS // LANES):
                lanes = slice(j * LANES, (j + 1) * LANES)
                assign = (
                    kern[rows, k0 + j * LANES:k0 + (j + 1) * LANES] * cref[j:j + 1, :]) * scale
                out_ref[rows, lanes] = (assign * float(TOTAL_PROTOS)).astype(jnp.bfloat16)
            return 0

        lax.fori_loop(0, ROWS // LANES, body, 0)

    def exchange_columns(it):
        for d in range(1, NX):
            start(colbuf.at[it, b], colbuf.at[it, b], col_rs.at[it],
                  device((b + d) % NX, y, z, c))
        peers = colbuf.at[it, pl.ds(0, NX - 1)]
        remote(peers, peers, col_rs.at[it], partner).wait_recv()
        total = (colbuf[it, 0] + colbuf[it, 1]) + (colbuf[it, 2] + colbuf[it, 3])
        cvec[...] = 1.0 / (float(TOTAL_PROTOS) * total)

    def plane_send(ref, rsem):
        offsets = [(dy, dz) for dy in range(NY) for dz in range(NZ) if dy or dz]
        offsets.sort(key=lambda o: -(min(o[0], NY - o[0]) + min(o[1], NZ - o[1])))
        for dy, dz in offsets:
            start(ref, ref, rsem, device(b, (y + dy) % NY, (z + dz) % NZ, c))

    def plane_wait(peers, rsem):
        remote(peers, peers, rsem, partner).wait_recv()

    def share(zs):
        for zz in zs:
            start(xg.at[:, zz], xp.at[:, zz], xp_rs, partner)

    @pl.when(c == 1)
    def _():
        own = load(v1_ref, xg.at[y, z, 1], local_sem.at[1])
        other = load(v2_ref, vstage, local_sem.at[2])
        normalize(1)
        own.wait()
        other.wait()
        enter()
        hand_over(1)
        far = NZ // 2
        loaded = [None]

        def work(k, *zs):
            if not zs:
                chunk_product(k, *loaded[k], 0)
                return
            loaded.append(zs)
            share(zs)
            chunk_load(k, *zs)
            chunk_product(k, *zs, 1)
            if k == 1:
                pl.semaphore_signal(go_sem, 1, device_id=partner, device_id_type=MESH)
                remote(pt.at[0], pt.at[0], pu_rs, partner).wait_recv()
            if k >= far - 1:
                chunk_product(k, *zs, 0)

        gather(1, work)
        for it in range(SINK_ITERS):
            if it > 0:
                column_pass(colbuf.at[it, b])
            exchange_columns(it)
            if it == SINK_ITERS - 1:
                start(cvec.at[pl.ds(0, 8)], svec, vec_rs.at[0], partner)
            row_pass(rowbuf.at[it, chip])
            plane_send(rowbuf.at[it, chip], row_rs.at[it])
            if it == 1:
                remote(xg, xp, xp_rs, partner).wait_recv()
                second_view(xp, 1)
                remote(pstat.at[0], sstat.at[0], vec_rs.at[4], partner).wait_recv()
                tbuf[chip] = pstat[0] + sstat[0]
                plane_send(tbuf.at[chip], t_rs)
            if it == SINK_ITERS - 1:
                cross_pass(COLS, cvec.at[pl.ds(8, 8)], False)
                remote(pstat.at[1], sstat.at[1], vec_rs.at[1], partner).wait_recv()
                xbuf[chip] = pstat[1] + sstat[1]
                plane_send(xbuf.at[chip], x_rs)
            plane_wait(rowbuf.at[it, pl.ds(0, NCHIP - 1)], row_rs.at[it])
            row_sums = jnp.sum(rowbuf[it], axis=0)
            rvec[...] = 1.0 / (float(TOTAL_ROWS) * row_sums)
            if it == SINK_ITERS - 1:
                start(rvec, lvec.at[0], vec_rs.at[2], partner)
            spread_rows(rvec)
        write_out(COLS, cvec.at[pl.ds(8, 8)])
        plane_wait(tbuf.at[pl.ds(0, NCHIP - 1)], t_rs)
        totals = jnp.log(jnp.sum(tbuf[...], axis=0))
        row_sums = jnp.sum(rowbuf[SINK_ITERS - 1], axis=0)
        plane_wait(xbuf.at[pl.ds(0, NCHIP - 1)], x_rs)
        loss = totals - jnp.sum(xbuf[...], axis=0) / row_sums
        loss_ref[...] = loss
        lvec[1] = loss
        start(lvec.at[1], lvec.at[1], vec_rs.at[3], partner)
        drain()

    @pl.when(c == 0)
    def _():
        own = load(v2_ref, xg.at[y, z, 0], local_sem.at[1])
        other = load(v1_ref, vstage, local_sem.at[2])
        normalize(0)
        own.wait()
        other.wait()
        enter()
        hand_over(0)
        start(pt.at[0], pt.at[0], pu_rs, partner)
        pl.semaphore_wait(go_sem, 1)
        gather(0, lambda k, *zs: share(zs))
        second_view(xg, 0)
        start(pstat.at[0], sstat.at[0], vec_rs.at[4], partner)
        remote(xg, xp, xp_rs, partner).wait_recv()
        kernel_block(xp, 0)
        remote(cvec.at[pl.ds(0, 8)], svec, vec_rs.at[0], partner).wait_recv()
        cross_pass(0, svec, True)
        start(pstat.at[1], sstat.at[1], vec_rs.at[1], partner)
        remote(rvec, lvec.at[0], vec_rs.at[2], partner).wait_recv()
        spread_rows(lvec.at[0])
        write_out(0, svec)
        remote(lvec.at[1], lvec.at[1], vec_rs.at[3], partner).wait_recv()
        loss_ref[...] = lvec[1]
        drain()


def local(view_codes, predictor_view_embeddings, prototypes):
    f32, bf16 = jnp.float32, jnp.bfloat16
    anywhere = pl.BlockSpec(memory_space=pltpu.HBM)
    vmem = pl.BlockSpec(memory_space=pltpu.VMEM)
    dma = pltpu.SemaphoreType.DMA
    assignments, loss = pl.pallas_call(
        swap_kernel,
        out_shape=(
            jax.ShapeDtypeStruct((ROWS, COLS), bf16),
            jax.ShapeDtypeStruct((8, LANES), f32),
        ),
        in_specs=[anywhere] * 3,
        out_specs=(vmem, vmem),
        scratch_shapes=[
            pltpu.VMEM((NY, NZ, 2, SHARD, ROWS), bf16),
            pltpu.VMEM((NY, NZ, 2, SHARD, ROWS), bf16),
            pltpu.VMEM((COLS, DIM), bf16),
            pltpu.VMEM((2, NY, NZ, 2 * SHARD, COLS), bf16),
            pltpu.VMEM((ROWS, 2 * COLS), f32),
            pltpu.VMEM((ROWS, COLS), f32),
            pltpu.VMEM((ROWS, DIM), bf16),
            pltpu.VMEM((SHARD, ROWS), bf16),
            pltpu.VMEM((8, ROWS), f32),
            pltpu.VMEM((ROWS, LANES), f32),
            pltpu.VMEM((ROWS, LANES), f32),
            pltpu.VMEM((ROWS, LANES), f32),
            pltpu.VMEM((SINK_ITERS, NX, 16, LANES), f32),
            pltpu.VMEM((SINK_ITERS, NCHIP, 8, LANES), f32),
            pltpu.VMEM((NCHIP, 8, LANES), f32),
            pltpu.VMEM((NCHIP, 8, LANES), f32),
            pltpu.VMEM((16, LANES), f32),
            pltpu.VMEM((8, LANES), f32),
            pltpu.VMEM((8, LANES), f32),
            pltpu.VMEM((2, 8, LANES), f32),
            pltpu.VMEM((2, 8, LANES), f32),
            pltpu.VMEM((2, 8, LANES), f32),
            pltpu.VMEM((8, LANES), f32),
            dma((3,)),
            dma((NY, NZ, 2)),
            dma(()),
            dma(()),
            dma(()),
            dma((SINK_ITERS,)),
            dma((SINK_ITERS,)),
            dma(()),
            dma(()),
            dma((5,)),
            pltpu.SemaphoreType.REGULAR,
        ],
        compiler_params=pltpu.CompilerParams(
            collective_id=0, has_side_effects=True, vmem_limit_bytes=48 << 20),
        name="swapped_sinkhorn",
    )(*[pltpu.with_memory_space_constraint(a, pltpu.HBM) for a in (
        view_codes.T, predictor_view_embeddings.T, prototypes)])
    return assignments, loss.reshape(ROWS)


def solution(mesh):
    placed = (P("batch", "proto"), P("batch", "proto"), P("proto", None))
    return jax.shard_map(
        local,
        mesh=mesh,
        in_specs=placed,
        out_specs=(P("batch", "proto"), P("batch")),
        check_vma=False,
    )
```

```python
import functools
import math

import jax
import jax.numpy as jnp
from jax import lax
from jax.experimental import pallas as pl
from jax.experimental.pallas import tpu as pltpu
from jax.sharding import PartitionSpec as P

SINK_ITERS = 3
EPSILON = 0.05
SOFTMAX_TEMP_VALUE = 0.1
LOG2E = math.log2(math.e)

MESH = pl.DeviceIdType.MESH
NX, NY, NZ = 4, 4, 8
NCHIP = NY * NZ
ROWS = 1024
COLS = 1024
DIM = 1024
SHARD = 16
LANES = 128
TOTAL_ROWS = 4096
TOTAL_PROTOS = 65536
GO_AT = 2


def swap_kernel(
    v1_ref, v2_ref, p_ref, out_ref, loss_ref,
    xg, xp, praw, pt, kern, s2, xb, vstage, squares, rscr, col_r, inv_col,
    colacc, rsum, colbuf, rowbuf, tbuf, xbuf, cvec, svec, rvec, lvec, sstat, pstat, inv_row2,
    local_sem, gather_rs, send_sem, xp_rs, pu_rs, col_rs, row_rs, t_rs, x_rs, vec_rs, go_sem,
):
    b = lax.axis_index("batch")
    q = lax.axis_index("proto")
    c = q % 2
    z = (q // 2) % NZ
    y = q // (2 * NZ)
    chip = y * NZ + z

    def device(bb, yy, zz, cc):
        return (bb, yy * (2 * NZ) + zz * 2 + cc)

    def at_y(d):
        return device(b, (y + d) % NY, z, c)

    def at_z(d):
        return device(b, y, (z + d) % NZ, c)

    partner = device(b, y, z, 1 - c)
    sent = []

    def remote(src, dst, rsem, dev):
        return pltpu.make_async_remote_copy(
            src_ref=src, dst_ref=dst, send_sem=send_sem, recv_sem=rsem,
            device_id=dev, device_id_type=MESH)

    def start(src, dst, rsem, dev):
        copy = remote(src, dst, rsem, dev)
        copy.start()
        sent.append(copy)

    def drain():
        for copy in sent:
            copy.wait_send()
        sent.clear()

    own_p = pltpu.make_async_copy(p_ref, praw, local_sem.at[0])

    def load(src, dst, sem):
        copy = pltpu.make_async_copy(src, dst, sem)
        copy.start()
        return copy

    barrier = pltpu.get_barrier_semaphore()
    greet = [partner]
    greet += [device((b + d) % NX, y, z, c) for d in range(1, NX)]
    near = [(d, 0) for d in (2, 1, 3)] + [(0, d) for d in (1, NZ - 1)]
    for cc in (c, 1 - c):
        greet += [device(b, (y + dy) % NY, (z + dz) % NZ, cc) for dy, dz in near]
    for dev in greet:
        pl.semaphore_signal(barrier, 1, device_id=dev, device_id_type=MESH)

    def enter():
        pl.semaphore_wait(barrier, len(greet))

    def normalize(slot):
        own_p.wait()

        def body(i, _):
            rows = pl.ds(pl.multiple_of(i * LANES, LANES), LANES)
            w = praw[rows, :].astype(jnp.float32)
            total = jnp.sum(w * w, axis=1, keepdims=True)
            unit = (w * lax.rsqrt(total + 1e-06)).astype(jnp.bfloat16)
            pt[slot, :, :, :, rows] = jnp.transpose(unit).reshape(NY, NZ, 2 * SHARD, LANES)
            return 0

        lax.fori_loop(0, COLS // LANES, body, 0)

    def put(yy, zz, h, dev):
        start(xg.at[yy, zz, h], xg.at[yy, zz, h], gather_rs.at[yy, zz, h], dev)

    def arrived(yy, zz, h):
        remote(xg.at[yy, zz, h], xg.at[yy, zz, h], gather_rs.at[yy, zz, h], partner).wait_recv()

    def hops(j, direction):
        far = NZ // 2
        if direction > 0:
            return far if j in (0, 1) else far - 1
        return far - 1 if j in (0, 1) else far

    def targets(h, steps):
        along_z = [(0, sign * st) for st in steps for sign in (1, -1)]
        along_y = [(2, 0), (1, 0), (3, 0)]
        return along_y + along_z if h == 0 else along_z + along_y

    def hand_over(h, steps):
        rsem = gather_rs.at[y, z, h]
        for dy, dz in targets(h, steps):
            start(vstage, xg.at[y, z, h], rsem,
                  device(b, (y + dy) % NY, (z + dz + NZ) % NZ, 1 - c))
        start(vstage, xg.at[y, z, h], rsem, partner)

    def first_puts(h, steps):
        for dy, dz in targets(h, steps):
            put(y, z, h, device(b, (y + dy) % NY, (z + dz + NZ) % NZ, c))

    def yj(j):
        return (y + j) % NY

    def zk(k):
        return (z + k + NZ) % NZ

    def ring(k, js, children):
        for direction in (1, -1):
            zz = zk(-direction * k)
            for j in js:
                for h in ((0, 1) if j == 0 else (0,)):
                    reach = hops(1 if h else j, direction)
                    if reach < k:
                        continue
                    arrived(yj(j), zz, h)
                    for st in children.get(k, ()):
                        if k + st <= reach:
                            put(yj(j), zz, h, at_z(zk(direction * st) - z + NZ))
                    if h:
                        for d in (2, 1, 3):
                            put(y, zz, 1, at_y(d))

    def local_units(steps):
        for i, st in enumerate(steps):
            for j in (1, 3, 2):
                if i == 0:
                    arrived(yj(j), z, 0)
                put(yj(j), z, 0, at_z(st))
                put(yj(j), z, 0, at_z(NZ - st))

    def finish(k, own, work):
        far = NZ // 2
        offsets = (k, NZ - k) if k < far else (0, far)
        for o in offsets:
            for j in (1, 3, 2):
                arrived(yj(j), zk(o), 1)
        if k == far:
            arrived(y, z, 1 - own)
        work(k, zk(offsets[0]), zk(offsets[1]))

    def gather(own, work, go):
        far = NZ // 2
        children = {k: (1,) for k in range(far)}
        ring(1, (0,), children)
        local_units((1,))
        for k in range(1, far + 1):
            if k < far:
                ring(k + 1, (0,), children)
                if k > 1:
                    work(k - 1)
            ring(k, (1, 3, 2), children)
            if k == GO_AT:
                go()
            finish(k, own, work)

    def row_squares(block):
        v = block.astype(jnp.float32)
        return jnp.sum((v * v).reshape(-1, 8, ROWS), axis=0)

    def spread(row, dst, g):
        dst[g * LANES:(g + 1) * LANES, :] = jnp.transpose(
            jnp.broadcast_to(row, (LANES, LANES)))

    def spread_scale(inv, factor):
        for g in range(ROWS // LANES):
            spread(inv[:, g * LANES:(g + 1) * LANES] * factor, inv_col, g)

    def inverse(sums):
        return lax.rsqrt(jnp.sum(sums, axis=0, keepdims=True) + 1e-06)

    def transpose_view(xt):
        sums = jnp.zeros((8, ROWS), jnp.float32)
        for kb in range(DIM // LANES):
            yy, z0 = kb // 2, (kb % 2) * 4
            block = xt[yy, z0:z0 + 4].reshape(LANES, ROWS)
            xb[:, kb * LANES:(kb + 1) * LANES] = jnp.transpose(block)
            sums += row_squares(block)
        return inverse(sums)

    NB = 256

    def chunk_load(k, z0, z1):
        sums = jnp.zeros((8, ROWS), jnp.float32)
        for i, zz in enumerate((z0, z1)):
            block = xg[:, zz].reshape(LANES, ROWS)
            at = (k - 1) * 2 * LANES + i * LANES
            xb[:, at:at + LANES] = jnp.transpose(block)
            sums += row_squares(block)
        if k > 1:
            sums += squares[...]
        squares[...] = sums
        if k == NZ // 2:
            spread_scale(inverse(sums), LOG2E / EPSILON)

    def chunk_product(k, z0, z1, slot):
        first, last = k == 1, k == NZ // 2
        depth = slice((k - 1) * 2 * LANES, k * 2 * LANES)
        for t in range(COLS // NB):
            lanes = slice(t * NB, (t + 1) * NB)
            rhs = jnp.concatenate([
                pt[slot, :, zz, :, lanes].reshape(LANES, NB) for zz in (z0, z1)], axis=0)
            cols = slice(slot * COLS + t * NB, slot * COLS + (t + 1) * NB)
            part = jnp.zeros((8, NB), jnp.float32)
            for m in range(ROWS // NB):
                mrows = slice(m * NB, (m + 1) * NB)
                s = jnp.dot(xb[mrows, depth], rhs, preferred_element_type=jnp.float32)
                if not first:
                    s = s + kern[mrows, cols]
                if last:
                    scale = inv_col[mrows, :]
                    s = jnp.exp2(s * jnp.concatenate([scale, scale], axis=1))
                    part += jnp.sum(s.reshape(NB // 8, 8, NB), axis=0)
                kern[mrows, cols] = s
            if last:
                total = jnp.sum(part, axis=0, keepdims=True)
                for u in range(NB // LANES):
                    row = t * (NB // LANES) + u
                    colbuf[0, slot, b, row:row + 1, :] = total[:, u * LANES:(u + 1) * LANES]

    MB = 512

    def products(slot, epilogue):
        def body(i, _):
            ncols = pl.ds(pl.multiple_of(i * NB, NB), NB)
            rhs = pt[slot, :, :, :, ncols].reshape(DIM, NB)
            for m in range(ROWS // MB):
                mrows = slice(m * MB, (m + 1) * MB)
                s = jnp.dot(xb[mrows, :], rhs, preferred_element_type=jnp.float32)
                epilogue(mrows, ncols, s)
            return 0

        lax.fori_loop(0, COLS // NB, body, 0)

    def kernel_block(xt, slot):
        spread_scale(transpose_view(xt), LOG2E / EPSILON)

        def epilogue(mrows, ncols, s):
            scale = inv_col[mrows, :]
            value = jnp.exp2(s * jnp.concatenate([scale, scale], axis=1))
            kern[mrows, ncols] = value
            s2[mrows, ncols] = s2[mrows, ncols] * value

        products(slot, epilogue)

    def gather_lanes(dst, first=0, count=ROWS // LANES):
        for g in range(count):
            at = (first + g) * LANES
            dst[g:g + 1, :] = jnp.sum(
                jnp.transpose(rscr[at:at + LANES, :]), axis=0, keepdims=True)

    def second_view(xt, slot):
        inv = transpose_view(xt)
        for g in range(ROWS // LANES):
            inv_row2[g:g + 1, :] = inv[:, g * LANES:(g + 1) * LANES]
        spread_scale(inv, LOG2E / SOFTMAX_TEMP_VALUE)
        rscr[...] = jnp.zeros((ROWS, LANES), jnp.float32)

        def epilogue(mrows, ncols, s):
            s2[mrows, ncols] = s
            scale = inv_col[mrows, :]
            e = jnp.exp2(s * jnp.concatenate([scale, scale], axis=1))
            rscr[mrows, :] += e[:, :LANES] + e[:, LANES:]

        products(slot, epilogue)
        gather_lanes(pstat.at[0])

    nj = COLS // LANES
    half_groups = ROWS // 16

    def column_sums(cols, g0, init):
        def body(g, accs):
            rows = pl.ds(pl.multiple_of(g * 8, 8), 8)
            r = col_r[rows, :]
            return tuple(
                acc + kern[rows, j * LANES:(j + 1) * LANES] * r for j, acc in zip(cols, accs))

        return lax.fori_loop(g0, g0 + half_groups, body, init, unroll=4)

    def columns_a():
        cols = range(2 * nj)
        zero = jnp.zeros((8, LANES), jnp.float32)
        for j, acc in zip(cols, column_sums(cols, 0, (zero,) * (2 * nj))):
            colacc[j] = acc

    def columns_b(it, slot):
        cols = range(slot * nj, (slot + 1) * nj)
        accs = column_sums(cols, half_groups, tuple(colacc[j] for j in cols))
        for j, acc in enumerate(accs):
            colbuf[it, slot, b, j:j + 1, :] = jnp.sum(acc, axis=0, keepdims=True)

    def rows_slot(slot, r0, count):
        def body(g, _):
            rows = pl.ds(pl.multiple_of(r0 + g * 64, 64), 64)
            acc = rscr[rows, :] if slot else jnp.zeros((64, LANES), jnp.float32)
            for j in range(slot * nj, (slot + 1) * nj):
                acc += kern[rows, j * LANES:(j + 1) * LANES] * cvec[j:j + 1, :]
            rscr[rows, :] = acc
            return 0

        lax.fori_loop(0, count // 64, body, 0, unroll=2)

    def cross_pass(k0, cref, ready):
        def body(g, _):
            rows = pl.ds(pl.multiple_of(g * 64, 64), 64)
            acc = jnp.zeros((64, LANES), jnp.float32)
            for j in range(COLS // LANES):
                term = s2[rows, j * LANES:(j + 1) * LANES] * cref[j:j + 1, :]
                if not ready:
                    term = term * kern[rows, k0 + j * LANES:k0 + (j + 1) * LANES]
                acc += term
            rscr[rows, :] = acc
            return 0

        lax.fori_loop(0, ROWS // 64, body, 0, unroll=2)
        gather_lanes(pstat.at[1])
        pstat[1] = pstat[1] * inv_row2[...] * (1.0 / SOFTMAX_TEMP_VALUE)

    def spread_rows(rows8):
        for g in range(ROWS // LANES):
            spread(rows8[g:g + 1, :], col_r, g)

    def weigh(k0, cref):
        def body(g, _):
            rows = pl.ds(pl.multiple_of(g * 64, 64), 64)
            for j in range(COLS // LANES):
                lanes = slice(k0 + j * LANES, k0 + (j + 1) * LANES)
                kern[rows, lanes] = kern[rows, lanes] * cref[j:j + 1, :]
            return 0

        lax.fori_loop(0, ROWS // 64, body, 0)

    def write_out(k0):
        def body(g, _):
            rows = pl.ds(pl.multiple_of(g * 64, 64), 64)
            scale = col_r[rows, :] * float(TOTAL_ROWS * TOTAL_PROTOS)
            for j in range(COLS // LANES):
                out_ref[rows, j * LANES:(j + 1) * LANES] = (
                    kern[rows, k0 + j * LANES:k0 + (j + 1) * LANES] * scale).astype(jnp.bfloat16)
            return 0

        lax.fori_loop(0, ROWS // 64, body, 0, unroll=2)

    def send_columns(it, slot):
        for d in (2, 1, 3):
            start(colbuf.at[it, slot, b], colbuf.at[it, slot, b], col_rs.at[it, slot],
                  device((b + d) % NX, y, z, c))

    def wait_columns(it, slot):
        peers = colbuf.at[it, slot, pl.ds(0, NX - 1)]
        remote(peers, peers, col_rs.at[it, slot], partner).wait_recv()
        total = (colbuf[it, slot, 0] + colbuf[it, slot, 1]) + (
            colbuf[it, slot, 2] + colbuf[it, slot, 3])
        cvec[slot * nj:(slot + 1) * nj, :] = 1.0 / (float(TOTAL_PROTOS) * total)

    def plane_send(ref, rsem):
        offsets = [(dy, dz) for dy in range(NY) for dz in range(NZ) if dy or dz]
        offsets.sort(key=lambda o: -(min(o[0], NY - o[0]) + min(o[1], NZ - o[1])))
        for dy, dz in offsets:
            start(ref, ref, rsem, device(b, (y + dy) % NY, (z + dz) % NZ, c))

    def plane_wait(peers, rsem):
        remote(peers, peers, rsem, partner).wait_recv()

    def share(zs):
        for zz in zs:
            start(xg.at[:, zz], xp.at[:, zz], xp_rs, partner)

    @pl.when(c == 1)
    def _():
        own = load(v1_ref, xg.at[y, z, 1], local_sem.at[1])
        other = load(v2_ref, vstage, local_sem.at[2])
        own_p.start()
        own.wait()
        other.wait()
        enter()
        first_puts(1, (1,))
        hand_over(1, (1,))
        normalize(1)

        def go():
            pl.semaphore_signal(go_sem, 1, device_id=partner, device_id_type=MESH)

        loaded = [None]

        def work(k, *zs):
            if not zs:
                if k == 1:
                    remote(pt.at[0], pt.at[0], pu_rs, partner).wait_recv()
                chunk_product(k, *loaded[k], 0)
                return
            loaded.append(zs)
            share(zs)
            chunk_load(k, *zs)
            for slot in (1, 0) if k >= NZ // 2 - 1 else (1,):
                chunk_product(k, *zs, slot)
                if k == NZ // 2:
                    send_columns(0, slot)

        gather(1, work, go)
        last = SINK_ITERS - 1
        for it in range(SINK_ITERS):
            if it > 0:
                columns_b(it, 0)
                send_columns(it, 0)
                columns_b(it, 1)
                send_columns(it, 1)
            wait_columns(it, 0)
            if it == last:
                start(cvec.at[pl.ds(0, 8)], svec, vec_rs.at[0], partner)
            rows_slot(0, 0, ROWS)
            wait_columns(it, 1)
            for half in range(2):
                rows_slot(1, half * (ROWS // 2), ROWS // 2)
                gather_lanes(rowbuf.at[it, half, chip], half * 4, 4)
                plane_send(rowbuf.at[it, half, chip], row_rs.at[it, half])
            if it == 1:
                remote(xg, xp, xp_rs, partner).wait_recv()
                second_view(xp, 1)
                remote(pstat.at[0], sstat.at[0], vec_rs.at[4], partner).wait_recv()
                tbuf[chip] = pstat[0] + sstat[0]
                plane_send(tbuf.at[chip], t_rs)
            if it == SINK_ITERS - 1:
                cross_pass(COLS, cvec.at[pl.ds(8, 8)], False)
                remote(pstat.at[1], sstat.at[1], vec_rs.at[1], partner).wait_recv()
                xbuf[chip] = pstat[1] + sstat[1]
                plane_send(xbuf.at[chip], x_rs)
                weigh(COLS, cvec.at[pl.ds(8, 8)])
            for half in range(2):
                plane_wait(rowbuf.at[it, half, pl.ds(0, NCHIP - 1)], row_rs.at[it, half])
                sums = jnp.sum(rowbuf[it, half], axis=0)
                rsum[half * 4:half * 4 + 4, :] = sums
                rvec[half * 4:half * 4 + 4, :] = 1.0 / (float(TOTAL_ROWS) * sums)
                if it == last and half:
                    start(rvec, lvec.at[0], vec_rs.at[2], partner)
                for g in range(half * 4, half * 4 + 4):
                    spread(rvec[g:g + 1, :], col_r, g)
                if it < last and not half:
                    columns_a()
        write_out(COLS)
        plane_wait(tbuf.at[pl.ds(0, NCHIP - 1)], t_rs)
        totals = jnp.log(jnp.sum(tbuf[...], axis=0))
        plane_wait(xbuf.at[pl.ds(0, NCHIP - 1)], x_rs)
        loss = totals - jnp.sum(xbuf[...], axis=0) / rsum[...]
        loss_ref[...] = loss
        lvec[1] = loss
        start(lvec.at[1], lvec.at[1], vec_rs.at[3], partner)
        drain()

    @pl.when(c == 0)
    def _():
        own = load(v2_ref, xg.at[y, z, 0], local_sem.at[1])
        other = load(v1_ref, vstage, local_sem.at[2])
        own_p.start()
        own.wait()
        other.wait()
        enter()
        hand_over(0, (1,))
        normalize(0)
        start(pt.at[0], pt.at[0], pu_rs, partner)
        pl.semaphore_wait(go_sem, 1)
        first_puts(0, (1,))
        gather(0, lambda k, *zs: share(zs), lambda: None)
        second_view(xg, 0)
        start(pstat.at[0], sstat.at[0], vec_rs.at[4], partner)
        remote(xg, xp, xp_rs, partner).wait_recv()
        kernel_block(xp, 0)
        remote(cvec.at[pl.ds(0, 8)], svec, vec_rs.at[0], partner).wait_recv()
        cross_pass(0, svec, True)
        start(pstat.at[1], sstat.at[1], vec_rs.at[1], partner)
        weigh(0, svec)
        remote(rvec, lvec.at[0], vec_rs.at[2], partner).wait_recv()
        spread_rows(lvec.at[0])
        write_out(0)
        remote(lvec.at[1], lvec.at[1], vec_rs.at[3], partner).wait_recv()
        loss_ref[...] = lvec[1]
        drain()


def local(view_codes, predictor_view_embeddings, prototypes):
    f32, bf16 = jnp.float32, jnp.bfloat16
    anywhere = pl.BlockSpec(memory_space=pltpu.HBM)
    vmem = pl.BlockSpec(memory_space=pltpu.VMEM)
    dma = pltpu.SemaphoreType.DMA
    assignments, loss = pl.pallas_call(
        swap_kernel,
        out_shape=(
            jax.ShapeDtypeStruct((ROWS, COLS), bf16),
            jax.ShapeDtypeStruct((8, LANES), f32),
        ),
        in_specs=[anywhere] * 3,
        out_specs=(vmem, vmem),
        scratch_shapes=[
            pltpu.VMEM((NY, NZ, 2, SHARD, ROWS), bf16),
            pltpu.VMEM((NY, NZ, 2, SHARD, ROWS), bf16),
            pltpu.VMEM((COLS, DIM), bf16),
            pltpu.VMEM((2, NY, NZ, 2 * SHARD, COLS), bf16),
            pltpu.VMEM((ROWS, 2 * COLS), f32),
            pltpu.VMEM((ROWS, COLS), f32),
            pltpu.VMEM((ROWS, DIM), bf16),
            pltpu.VMEM((SHARD, ROWS), bf16),
            pltpu.VMEM((8, ROWS), f32),
            pltpu.VMEM((ROWS, LANES), f32),
            pltpu.VMEM((ROWS, LANES), f32),
            pltpu.VMEM((ROWS, LANES), f32),
            pltpu.VMEM((16, 8, LANES), f32),
            pltpu.VMEM((8, LANES), f32),
            pltpu.VMEM((SINK_ITERS, 2, NX, 8, LANES), f32),
            pltpu.VMEM((SINK_ITERS, 2, NCHIP, 4, LANES), f32),
            pltpu.VMEM((NCHIP, 8, LANES), f32),
            pltpu.VMEM((NCHIP, 8, LANES), f32),
            pltpu.VMEM((16, LANES), f32),
            pltpu.VMEM((8, LANES), f32),
            pltpu.VMEM((8, LANES), f32),
            pltpu.VMEM((2, 8, LANES), f32),
            pltpu.VMEM((2, 8, LANES), f32),
            pltpu.VMEM((2, 8, LANES), f32),
            pltpu.VMEM((8, LANES), f32),
            dma((3,)),
            dma((NY, NZ, 2)),
            dma(()),
            dma(()),
            dma(()),
            dma((SINK_ITERS, 2)),
            dma((SINK_ITERS, 2)),
            dma(()),
            dma(()),
            dma((5,)),
            pltpu.SemaphoreType.REGULAR,
        ],
        compiler_params=pltpu.CompilerParams(
            collective_id=0, has_side_effects=True, vmem_limit_bytes=48 << 20),
        name="swapped_sinkhorn",
    )(*[pltpu.with_memory_space_constraint(a, pltpu.HBM) for a in (
        view_codes.T, predictor_view_embeddings.T, prototypes)])
    return assignments, loss.reshape(ROWS)


def solution(mesh):
    placed = (P("batch", "proto"), P("batch", "proto"), P("proto", None))
    return jax.shard_map(
        local,
        mesh=mesh,
        in_specs=placed,
        out_specs=(P("batch", "proto"), P("batch")),
        check_vma=False,
    )
```

```python
import functools
import math

import jax
import jax.numpy as jnp
from jax import lax
from jax.experimental import pallas as pl
from jax.experimental.pallas import tpu as pltpu
from jax.sharding import PartitionSpec as P

SINK_ITERS = 3
EPSILON = 0.05
SOFTMAX_TEMP_VALUE = 0.1
LOG2E = math.log2(math.e)

MESH = pl.DeviceIdType.MESH
NX, NY, NZ = 4, 4, 8
NCHIP = NY * NZ
ROWS = 1024
COLS = 1024
DIM = 1024
SHARD = 16
LANES = 128
TOTAL_ROWS = 4096
TOTAL_PROTOS = 65536
GO_AT = 2


def swap_kernel(
    v1_ref, v2_ref, p_ref, out_ref, loss_ref,
    xg, xp, praw, pt, kern, s2, xb, vstage, squares, rscr, col_r, inv_col,
    colacc, rsum, colbuf, rowbuf, tbuf, xbuf, cvec, svec, rvec, lvec, sstat, pstat, inv_row2,
    local_sem, gather_rs, send_sem, xp_rs, pu_rs, col_rs, row_rs, t_rs, x_rs, vec_rs, go_sem,
):
    b = lax.axis_index("batch")
    q = lax.axis_index("proto")
    c = q % 2
    z = (q // 2) % NZ
    y = q // (2 * NZ)
    chip = y * NZ + z

    def device(bb, yy, zz, cc):
        return (bb, yy * (2 * NZ) + zz * 2 + cc)

    def at_y(d):
        return device(b, (y + d) % NY, z, c)

    def at_z(d):
        return device(b, y, (z + d) % NZ, c)

    partner = device(b, y, z, 1 - c)
    sent = []

    def remote(src, dst, rsem, dev):
        return pltpu.make_async_remote_copy(
            src_ref=src, dst_ref=dst, send_sem=send_sem, recv_sem=rsem,
            device_id=dev, device_id_type=MESH)

    def start(src, dst, rsem, dev):
        copy = remote(src, dst, rsem, dev)
        copy.start()
        sent.append(copy)

    def drain():
        for copy in sent:
            copy.wait_send()
        sent.clear()

    own_p = pltpu.make_async_copy(p_ref, praw, local_sem.at[0])

    def load(src, dst, sem):
        copy = pltpu.make_async_copy(src, dst, sem)
        copy.start()
        return copy

    barrier = pltpu.get_barrier_semaphore()
    greet = [partner]
    greet += [device((b + d) % NX, y, z, c) for d in range(1, NX)]
    near = [(d, 0) for d in (2, 1, 3)] + [(0, d) for d in (1, NZ - 1)]
    for cc in (c, 1 - c):
        greet += [device(b, (y + dy) % NY, (z + dz) % NZ, cc) for dy, dz in near]
    for dev in greet:
        pl.semaphore_signal(barrier, 1, device_id=dev, device_id_type=MESH)

    def enter():
        pl.semaphore_wait(barrier, len(greet))

    def normalize(slot):
        own_p.wait()

        def body(i, _):
            rows = pl.ds(pl.multiple_of(i * LANES, LANES), LANES)
            w = praw[rows, :].astype(jnp.float32)
            total = jnp.sum(w * w, axis=1, keepdims=True)
            unit = (w * lax.rsqrt(total + 1e-06)).astype(jnp.bfloat16)
            pt[slot, :, :, :, rows] = jnp.transpose(unit).reshape(NY, NZ, 2 * SHARD, LANES)
            return 0

        lax.fori_loop(0, COLS // LANES, body, 0)

    def put(yy, zz, h, dev):
        start(xg.at[yy, zz, h], xg.at[yy, zz, h], gather_rs.at[yy, zz, h], dev)

    def arrived(yy, zz, h):
        remote(xg.at[yy, zz, h], xg.at[yy, zz, h], gather_rs.at[yy, zz, h], partner).wait_recv()

    def hops(j, direction):
        far = NZ // 2
        if direction > 0:
            return far if j in (0, 1) else far - 1
        return far - 1 if j in (0, 1) else far

    def targets(h, steps):
        along_z = [(0, sign * st) for st in steps for sign in (1, -1)]
        along_y = [(2, 0), (1, 0), (3, 0)]
        return along_y + along_z if h == 0 else along_z + along_y

    def hand_over(h, steps):
        rsem = gather_rs.at[y, z, h]
        for dy, dz in targets(h, steps):
            start(vstage, xg.at[y, z, h], rsem,
                  device(b, (y + dy) % NY, (z + dz + NZ) % NZ, 1 - c))
        start(vstage, xg.at[y, z, h], rsem, partner)

    def first_puts(h, steps):
        for dy, dz in targets(h, steps):
            put(y, z, h, device(b, (y + dy) % NY, (z + dz + NZ) % NZ, c))

    def yj(j):
        return (y + j) % NY

    def zk(k):
        return (z + k + NZ) % NZ

    def ring(k, js, children):
        for direction in (1, -1):
            zz = zk(-direction * k)
            for j in js:
                for h in ((0, 1) if j == 0 else (0,)):
                    reach = hops(1 if h else j, direction)
                    if reach < k:
                        continue
                    arrived(yj(j), zz, h)
                    for st in children.get(k, ()):
                        if k + st <= reach:
                            put(yj(j), zz, h, at_z(zk(direction * st) - z + NZ))
                    if h:
                        for d in (2, 1, 3):
                            put(y, zz, 1, at_y(d))

    def local_units(steps):
        for i, st in enumerate(steps):
            for j in (1, 3, 2):
                if i == 0:
                    arrived(yj(j), z, 0)
                put(yj(j), z, 0, at_z(st))
                put(yj(j), z, 0, at_z(NZ - st))

    def finish(k, own, work):
        far = NZ // 2
        offsets = (k, NZ - k) if k < far else (0, far)
        ready = {far - 1: offsets + (0,), far: (far,)}.get(k, offsets)
        for o in ready:
            for j in (1, 3, 2):
                arrived(yj(j), zk(o), 1)
        if k == far - 1:
            arrived(y, z, 1 - own)
        work(k, zk(offsets[0]), zk(offsets[1]))

    def gather(own, work, go):
        far = NZ // 2
        children = {k: (1,) for k in range(far)}
        ring(1, (0,), children)
        local_units((1,))
        for k in range(1, far + 1):
            if k < far:
                ring(k + 1, (0,), children)
                if k > 1:
                    work(k - 1)
            ring(k, (1, 3, 2), children)
            if k == GO_AT:
                go()
            finish(k, own, work)

    def row_squares(block):
        v = block.astype(jnp.float32)
        return jnp.sum((v * v).reshape(-1, 8, ROWS), axis=0)

    def spread(row, dst, g):
        dst[g * LANES:(g + 1) * LANES, :] = jnp.transpose(
            jnp.broadcast_to(row, (LANES, LANES)))

    def spread_scale(inv, factor):
        for g in range(ROWS // LANES):
            spread(inv[:, g * LANES:(g + 1) * LANES] * factor, inv_col, g)

    def inverse(sums):
        return lax.rsqrt(jnp.sum(sums, axis=0, keepdims=True) + 1e-06)

    def transpose_view(xt):
        sums = jnp.zeros((8, ROWS), jnp.float32)
        for kb in range(DIM // LANES):
            yy, z0 = kb // 2, (kb % 2) * 4
            block = xt[yy, z0:z0 + 4].reshape(LANES, ROWS)
            xb[:, kb * LANES:(kb + 1) * LANES] = jnp.transpose(block)
            sums += row_squares(block)
        return inverse(sums)

    NB = 256

    def chunk_load(k, pieces):
        sums = jnp.zeros((8, ROWS), jnp.float32)
        for i, zz in pieces:
            block = xg[:, zz].reshape(LANES, ROWS)
            at = (k - 1) * 2 * LANES + i * LANES
            xb[:, at:at + LANES] = jnp.transpose(block)
            sums += row_squares(block)
        if k > 1:
            sums += squares[...]
        squares[...] = sums
        if k == NZ // 2 and pieces[-1][0] == 1:
            spread_scale(inverse(sums), LOG2E / EPSILON)

    def chunk_product(k, z0, z1, slot):
        first, last = k == 1, k == NZ // 2
        depth = slice((k - 1) * 2 * LANES, k * 2 * LANES)
        for t in range(COLS // NB):
            lanes = slice(t * NB, (t + 1) * NB)
            rhs = jnp.concatenate([
                pt[slot, :, zz, :, lanes].reshape(LANES, NB) for zz in (z0, z1)], axis=0)
            cols = slice(slot * COLS + t * NB, slot * COLS + (t + 1) * NB)
            part = jnp.zeros((8, NB), jnp.float32)
            for m in range(ROWS // NB):
                mrows = slice(m * NB, (m + 1) * NB)
                s = jnp.dot(xb[mrows, depth], rhs, preferred_element_type=jnp.float32)
                if not first:
                    s = s + kern[mrows, cols]
                if last:
                    scale = inv_col[mrows, :]
                    s = jnp.exp2(s * jnp.concatenate([scale, scale], axis=1))
                    part += jnp.sum(s.reshape(NB // 8, 8, NB), axis=0)
                kern[mrows, cols] = s
            if last:
                total = jnp.sum(part, axis=0, keepdims=True)
                for u in range(NB // LANES):
                    row = t * (NB // LANES) + u
                    colbuf[0, slot, b, row:row + 1, :] = total[:, u * LANES:(u + 1) * LANES]

    MB = 512

    def products(slot, epilogue):
        def body(i, _):
            ncols = pl.ds(pl.multiple_of(i * NB, NB), NB)
            rhs = pt[slot, :, :, :, ncols].reshape(DIM, NB)
            for m in range(ROWS // MB):
                mrows = slice(m * MB, (m + 1) * MB)
                s = jnp.dot(xb[mrows, :], rhs, preferred_element_type=jnp.float32)
                epilogue(mrows, ncols, s)
            return 0

        lax.fori_loop(0, COLS // NB, body, 0)

    def kernel_block(xt, slot):
        spread_scale(transpose_view(xt), LOG2E / EPSILON)

        def epilogue(mrows, ncols, s):
            scale = inv_col[mrows, :]
            value = jnp.exp2(s * jnp.concatenate([scale, scale], axis=1))
            kern[mrows, ncols] = value
            s2[mrows, ncols] = s2[mrows, ncols] * value

        products(slot, epilogue)

    def gather_lanes(dst, first=0, count=ROWS // LANES):
        for g in range(count):
            at = (first + g) * LANES
            dst[g:g + 1, :] = jnp.sum(
                jnp.transpose(rscr[at:at + LANES, :]), axis=0, keepdims=True)

    def second_view(xt, slot):
        inv = transpose_view(xt)
        for g in range(ROWS // LANES):
            inv_row2[g:g + 1, :] = inv[:, g * LANES:(g + 1) * LANES]
        spread_scale(inv, LOG2E / SOFTMAX_TEMP_VALUE)
        rscr[...] = jnp.zeros((ROWS, LANES), jnp.float32)

        def epilogue(mrows, ncols, s):
            s2[mrows, ncols] = s
            scale = inv_col[mrows, :]
            e = jnp.exp2(s * jnp.concatenate([scale, scale], axis=1))
            rscr[mrows, :] += e[:, :LANES] + e[:, LANES:]

        products(slot, epilogue)
        gather_lanes(pstat.at[0])

    nj = COLS // LANES
    half_groups = ROWS // 16

    def column_sums(cols, g0, init):
        def body(g, accs):
            rows = pl.ds(pl.multiple_of(g * 8, 8), 8)
            r = col_r[rows, :]
            return tuple(
                acc + kern[rows, j * LANES:(j + 1) * LANES] * r for j, acc in zip(cols, accs))

        return lax.fori_loop(g0, g0 + half_groups, body, init, unroll=4)

    def columns_a():
        cols = range(2 * nj)
        zero = jnp.zeros((8, LANES), jnp.float32)
        for j, acc in zip(cols, column_sums(cols, 0, (zero,) * (2 * nj))):
            colacc[j] = acc

    def columns_b(it, slot):
        cols = range(slot * nj, (slot + 1) * nj)
        accs = column_sums(cols, half_groups, tuple(colacc[j] for j in cols))
        for j, acc in enumerate(accs):
            colbuf[it, slot, b, j:j + 1, :] = jnp.sum(acc, axis=0, keepdims=True)

    def rows_slot(slot, r0, count):
        def body(g, _):
            rows = pl.ds(pl.multiple_of(r0 + g * 64, 64), 64)
            acc = rscr[rows, :] if slot else jnp.zeros((64, LANES), jnp.float32)
            for j in range(slot * nj, (slot + 1) * nj):
                acc += kern[rows, j * LANES:(j + 1) * LANES] * cvec[j:j + 1, :]
            rscr[rows, :] = acc
            return 0

        lax.fori_loop(0, count // 64, body, 0, unroll=2)

    def cross_pass(k0, cref, ready):
        def body(g, _):
            rows = pl.ds(pl.multiple_of(g * 64, 64), 64)
            acc = jnp.zeros((64, LANES), jnp.float32)
            for j in range(COLS // LANES):
                term = s2[rows, j * LANES:(j + 1) * LANES] * cref[j:j + 1, :]
                if not ready:
                    term = term * kern[rows, k0 + j * LANES:k0 + (j + 1) * LANES]
                acc += term
            rscr[rows, :] = acc
            return 0

        lax.fori_loop(0, ROWS // 64, body, 0, unroll=2)
        gather_lanes(pstat.at[1])
        pstat[1] = pstat[1] * inv_row2[...] * (1.0 / SOFTMAX_TEMP_VALUE)

    def spread_rows(rows8):
        for g in range(ROWS // LANES):
            spread(rows8[g:g + 1, :], col_r, g)

    def weigh(k0, cref):
        def body(g, _):
            rows = pl.ds(pl.multiple_of(g * 64, 64), 64)
            for j in range(COLS // LANES):
                lanes = slice(k0 + j * LANES, k0 + (j + 1) * LANES)
                kern[rows, lanes] = kern[rows, lanes] * cref[j:j + 1, :]
            return 0

        lax.fori_loop(0, ROWS // 64, body, 0)

    def write_out(k0):
        def body(g, _):
            rows = pl.ds(pl.multiple_of(g * 64, 64), 64)
            scale = col_r[rows, :] * float(TOTAL_ROWS * TOTAL_PROTOS)
            for j in range(COLS // LANES):
                out_ref[rows, j * LANES:(j + 1) * LANES] = (
                    kern[rows, k0 + j * LANES:k0 + (j + 1) * LANES] * scale).astype(jnp.bfloat16)
            return 0

        lax.fori_loop(0, ROWS // 64, body, 0, unroll=2)

    def send_columns(it, slot):
        for d in (2, 1, 3):
            start(colbuf.at[it, slot, b], colbuf.at[it, slot, b], col_rs.at[it, slot],
                  device((b + d) % NX, y, z, c))

    def wait_columns(it, slot):
        peers = colbuf.at[it, slot, pl.ds(0, NX - 1)]
        remote(peers, peers, col_rs.at[it, slot], partner).wait_recv()
        total = (colbuf[it, slot, 0] + colbuf[it, slot, 1]) + (
            colbuf[it, slot, 2] + colbuf[it, slot, 3])
        cvec[slot * nj:(slot + 1) * nj, :] = 1.0 / (float(TOTAL_PROTOS) * total)

    def plane_send(ref, rsem):
        offsets = [(dy, dz) for dy in range(NY) for dz in range(NZ) if dy or dz]
        offsets.sort(key=lambda o: -(min(o[0], NY - o[0]) + min(o[1], NZ - o[1])))
        for dy, dz in offsets:
            start(ref, ref, rsem, device(b, (y + dy) % NY, (z + dz) % NZ, c))

    def plane_wait(peers, rsem):
        remote(peers, peers, rsem, partner).wait_recv()

    def share(zs):
        for zz in zs:
            start(xg.at[:, zz], xp.at[:, zz], xp_rs, partner)

    @pl.when(c == 1)
    def _():
        own = load(v1_ref, xg.at[y, z, 1], local_sem.at[1])
        other = load(v2_ref, vstage, local_sem.at[2])
        own_p.start()
        own.wait()
        other.wait()
        enter()
        first_puts(1, (1,))
        hand_over(1, (1,))
        normalize(1)

        def go():
            pl.semaphore_signal(go_sem, 1, device_id=partner, device_id_type=MESH)

        loaded = [None]

        def work(k, *zs):
            if not zs:
                if k == 1:
                    remote(pt.at[0], pt.at[0], pu_rs, partner).wait_recv()
                chunk_product(k, *loaded[k], 0)
                return
            loaded.append(zs)
            share(zs)
            pieces = list(enumerate(zs))
            chunk_load(k, pieces[1:] if k == NZ // 2 else pieces)
            for slot in (1, 0) if k >= NZ // 2 - 1 else (1,):
                chunk_product(k, *zs, slot)
                if k == NZ // 2:
                    send_columns(0, slot)
            if k == NZ // 2 - 1:
                chunk_load(k + 1, [(0, z)])

        gather(1, work, go)
        last = SINK_ITERS - 1
        for it in range(SINK_ITERS):
            if it > 0:
                columns_b(it, 0)
                send_columns(it, 0)
                columns_b(it, 1)
                send_columns(it, 1)
            wait_columns(it, 0)
            if it == last:
                start(cvec.at[pl.ds(0, 8)], svec, vec_rs.at[0], partner)
            rows_slot(0, 0, ROWS)
            wait_columns(it, 1)
            for half in range(2):
                rows_slot(1, half * (ROWS // 2), ROWS // 2)
                gather_lanes(rowbuf.at[it, half, chip], half * 4, 4)
                plane_send(rowbuf.at[it, half, chip], row_rs.at[it, half])
            if it == 1:
                remote(xg, xp, xp_rs, partner).wait_recv()
                second_view(xp, 1)
                remote(pstat.at[0], sstat.at[0], vec_rs.at[4], partner).wait_recv()
                tbuf[chip] = pstat[0] + sstat[0]
                plane_send(tbuf.at[chip], t_rs)
            if it == SINK_ITERS - 1:
                cross_pass(COLS, cvec.at[pl.ds(8, 8)], False)
                remote(pstat.at[1], sstat.at[1], vec_rs.at[1], partner).wait_recv()
                xbuf[chip] = pstat[1] + sstat[1]
                plane_send(xbuf.at[chip], x_rs)
                weigh(COLS, cvec.at[pl.ds(8, 8)])
            for half in range(2):
                plane_wait(rowbuf.at[it, half, pl.ds(0, NCHIP - 1)], row_rs.at[it, half])
                sums = jnp.sum(rowbuf[it, half], axis=0)
                rsum[half * 4:half * 4 + 4, :] = sums
                rvec[half * 4:half * 4 + 4, :] = 1.0 / (float(TOTAL_ROWS) * sums)
                if it == last and half:
                    start(rvec, lvec.at[0], vec_rs.at[2], partner)
                for g in range(half * 4, half * 4 + 4):
                    spread(rvec[g:g + 1, :], col_r, g)
                if it < last and not half:
                    columns_a()
        write_out(COLS)
        plane_wait(tbuf.at[pl.ds(0, NCHIP - 1)], t_rs)
        totals = jnp.log(jnp.sum(tbuf[...], axis=0))
        plane_wait(xbuf.at[pl.ds(0, NCHIP - 1)], x_rs)
        loss = totals - jnp.sum(xbuf[...], axis=0) / rsum[...]
        loss_ref[...] = loss
        lvec[1] = loss
        start(lvec.at[1], lvec.at[1], vec_rs.at[3], partner)
        drain()

    @pl.when(c == 0)
    def _():
        own = load(v2_ref, xg.at[y, z, 0], local_sem.at[1])
        other = load(v1_ref, vstage, local_sem.at[2])
        own_p.start()
        own.wait()
        other.wait()
        enter()
        hand_over(0, (1,))
        normalize(0)
        start(pt.at[0], pt.at[0], pu_rs, partner)
        pl.semaphore_wait(go_sem, 1)
        first_puts(0, (1,))
        gather(0, lambda k, *zs: share(zs), lambda: None)
        second_view(xg, 0)
        start(pstat.at[0], sstat.at[0], vec_rs.at[4], partner)
        remote(xg, xp, xp_rs, partner).wait_recv()
        kernel_block(xp, 0)
        remote(cvec.at[pl.ds(0, 8)], svec, vec_rs.at[0], partner).wait_recv()
        cross_pass(0, svec, True)
        start(pstat.at[1], sstat.at[1], vec_rs.at[1], partner)
        weigh(0, svec)
        remote(rvec, lvec.at[0], vec_rs.at[2], partner).wait_recv()
        spread_rows(lvec.at[0])
        write_out(0)
        remote(lvec.at[1], lvec.at[1], vec_rs.at[3], partner).wait_recv()
        loss_ref[...] = lvec[1]
        drain()


def local(view_codes, predictor_view_embeddings, prototypes):
    f32, bf16 = jnp.float32, jnp.bfloat16
    anywhere = pl.BlockSpec(memory_space=pltpu.HBM)
    vmem = pl.BlockSpec(memory_space=pltpu.VMEM)
    dma = pltpu.SemaphoreType.DMA
    assignments, loss = pl.pallas_call(
        swap_kernel,
        out_shape=(
            jax.ShapeDtypeStruct((ROWS, COLS), bf16),
            jax.ShapeDtypeStruct((8, LANES), f32),
        ),
        in_specs=[anywhere] * 3,
        out_specs=(vmem, vmem),
        scratch_shapes=[
            pltpu.VMEM((NY, NZ, 2, SHARD, ROWS), bf16),
            pltpu.VMEM((NY, NZ, 2, SHARD, ROWS), bf16),
            pltpu.VMEM((COLS, DIM), bf16),
            pltpu.VMEM((2, NY, NZ, 2 * SHARD, COLS), bf16),
            pltpu.VMEM((ROWS, 2 * COLS), f32),
            pltpu.VMEM((ROWS, COLS), f32),
            pltpu.VMEM((ROWS, DIM), bf16),
            pltpu.VMEM((SHARD, ROWS), bf16),
            pltpu.VMEM((8, ROWS), f32),
            pltpu.VMEM((ROWS, LANES), f32),
            pltpu.VMEM((ROWS, LANES), f32),
            pltpu.VMEM((ROWS, LANES), f32),
            pltpu.VMEM((16, 8, LANES), f32),
            pltpu.VMEM((8, LANES), f32),
            pltpu.VMEM((SINK_ITERS, 2, NX, 8, LANES), f32),
            pltpu.VMEM((SINK_ITERS, 2, NCHIP, 4, LANES), f32),
            pltpu.VMEM((NCHIP, 8, LANES), f32),
            pltpu.VMEM((NCHIP, 8, LANES), f32),
            pltpu.VMEM((16, LANES), f32),
            pltpu.VMEM((8, LANES), f32),
            pltpu.VMEM((8, LANES), f32),
            pltpu.VMEM((2, 8, LANES), f32),
            pltpu.VMEM((2, 8, LANES), f32),
            pltpu.VMEM((2, 8, LANES), f32),
            pltpu.VMEM((8, LANES), f32),
            dma((3,)),
            dma((NY, NZ, 2)),
            dma(()),
            dma(()),
            dma(()),
            dma((SINK_ITERS, 2)),
            dma((SINK_ITERS, 2)),
            dma(()),
            dma(()),
            dma((5,)),
            pltpu.SemaphoreType.REGULAR,
        ],
        compiler_params=pltpu.CompilerParams(
            collective_id=0, has_side_effects=True, vmem_limit_bytes=48 << 20),
        name="swapped_sinkhorn",
    )(*[pltpu.with_memory_space_constraint(a, pltpu.HBM) for a in (
        view_codes.T, predictor_view_embeddings.T, prototypes)])
    return assignments, loss.reshape(ROWS)


def solution(mesh):
    placed = (P("batch", "proto"), P("batch", "proto"), P("proto", None))
    return jax.shard_map(
        local,
        mesh=mesh,
        in_specs=placed,
        out_specs=(P("batch", "proto"), P("batch")),
        check_vma=False,
    )
```
